32 devices in a mesh: dp: 8 (over z, x), seq: 4 (over y, core).
Axes of the slice: x: 2, y: 2, z: 4, core: 2. Of those that a mesh axis runs over, the one named last changes fastest.
Arguments:
- inputs: bfloat16 [4096, 1024], P(('dp', 'seq')), may hold values from -6 to 6
- gain_attn: bfloat16 [1024], P('dp'), may hold values from 0.25 to 1.75
- w_qkv: bfloat16 [1024, 3072], P('dp'), may hold values from -0.1875 to 0.1875
- b_qkv: bfloat16 [3072], P('dp'), may hold values from -5.5 to 5.5, as said below
- w_out: bfloat16 [1024, 1024], P('dp'), may hold values from -0.5 to 0.5
- gain_mlp: bfloat16 [1024], P('dp'), may hold values from 0.25 to 1.75
- w_gate: bfloat16 [1024, 2816], P('dp'), may hold values from -0.1875 to 0.1875
- w_up: bfloat16 [1024, 2816], P('dp'), may hold values from -0.1875 to 0.1875
- w_down: bfloat16 [2816, 1024], P('dp'), may hold values from -0.109375 to 0.109375
- cotangent: bfloat16 [4096, 1024], P(('dp', 'seq')), may hold values from -6 to 6
Outputs:
- output: bfloat16 [4096, 1024], P(('dp', 'seq'))
- grad_inputs: float32 [4096, 1024], P(('dp', 'seq'))
- grad_gain_attn: float32 [1024], P('dp')
- grad_w_qkv: float32 [1024, 3072], P('dp')
- grad_b_qkv: float32 [3072], P('dp')
- grad_w_out: float32 [1024, 1024], P('dp')
- grad_gain_mlp: float32 [1024], P('dp')
- grad_w_gate: float32 [1024, 2816], P('dp')
- grad_w_up: float32 [1024, 2816], P('dp')
- grad_w_down: float32 [2816, 1024], P('dp')
The draws below stay inside these ranges and needn't reach their ends.
Inputs may be any that keep to these rules, and one draw needn't show every extreme that they name: `b_qkv`: entries of the joint projection's bias.
All inputs are finite; a program needn't handle non-finite values.
Results may differ from the reference program's by a relative error of at most 0.02.
The reference program's roundings to bfloat16 on the way count: a program that leaves them out, or rounds other values in their place, can miss the bound.
Values may be sent and summed in bfloat16 or wider, within the bound.
A program may use at most 192 MiB of HBM per device.

```python
import math
import jax
import jax.numpy as jnp
from jax import lax

D = 1024
FF = 2816
HEADS = 16
KV_HEADS = 16
HEAD_DIM = 64
QDIM = 1024
KVDIM = 1024
QKV = 3072
SEQ_LEN = 512
TOKENS = 4096
N_DP = 8


def draw_b_qkv(key, part):
    base_key = jax.random.fold_in(key, 0)
    return jnp.clip(0.5 * jax.random.normal(base_key, (QKV,), jnp.float32), -3.0, 3.0).astype(jnp.bfloat16)


def level_of(key, shape, cuts, low, largest):
    level = 1.0
    for dim, parts in cuts:
        draws = jax.random.uniform(jax.random.fold_in(jax.random.fold_in(key, 6), dim), (parts,), jnp.float32, low / len(cuts), largest / len(cuts))
        level = level * jnp.repeat(jnp.exp(draws), shape[dim] // parts).reshape((-1,) + (1,) * (len(shape) - 1 - dim))
    return level


def centred(stream_key, dims, scale, bound, pieces=(), kind=jnp.bfloat16):
    entries = scale * jax.random.normal(stream_key, dims, jnp.float32)
    if pieces:
        entries = entries * level_of(stream_key, dims, pieces, -0.22, 0.18)
    return jnp.clip(entries, -bound, bound).astype(kind)


def setup_inputs(seed: int = 0) -> dict:
    keys = jax.random.split(jax.random.key(seed), 11)
    return {
        "inputs": centred(keys[0], (TOKENS, D), 1.0, 6.0, ((0, 32),)),
        "gain_attn": jnp.clip(1.0 + 0.15 * jax.random.normal(keys[1], (D,), jnp.float32), 0.25, 1.75).astype(jnp.bfloat16),
        "w_qkv": centred(keys[2], (D, QKV), D ** -0.5, 0.1875, ((0, 8),)),
        "b_qkv": draw_b_qkv(jax.random.fold_in(keys[10], 71), 0),
        "w_out": centred(keys[4], (QDIM, D), (QDIM // 8) ** -0.5, 0.5, ((0, 8),)),
        "gain_mlp": jnp.clip(1.0 + 0.15 * jax.random.normal(keys[5], (D,), jnp.float32), 0.25, 1.75).astype(jnp.bfloat16),
        "w_gate": centred(keys[6], (D, FF), D ** -0.5, 0.1875, ((0, 8),)),
        "w_up": centred(keys[7], (D, FF), D ** -0.5, 0.1875, ((0, 8),)),
        "w_down": centred(keys[8], (FF, D), FF ** -0.5, 0.109375, ((0, 8),)),
        "cotangent": centred(keys[9], (TOKENS, D), 1.0, 6.0, ((0, 32),)),
    }


NORM_EPS = 1e-06
ROPE_BASE = 1000000.0
MASK_LOW = -1000000000.0
HIGHEST = lax.Precision.HIGHEST

@jax.custom_vjp
def low(v):
    return lax.optimization_barrier(v.astype(jnp.bfloat16)).astype(jnp.float32)

@jax.custom_vjp
def low_back(v):
    return v

def low_keep(v):
    return (low(v), None)

def low_pass(kept, grad):
    return (grad,)

def back_keep(v):
    return (v, None)

def back_low(kept, grad):
    return (low(grad),)
low.defvjp(low_keep, low_pass)
low_back.defvjp(back_keep, back_low)

def rms_scale(signal, gain_vec):
    return signal * lax.rsqrt(lax.optimization_barrier(jnp.mean(signal * signal, axis=-1, keepdims=True)) + NORM_EPS) * gain_vec

def rotate(signal, cosine_tab, sine_tab):
    half_dim = signal.shape[-1] // 2
    turned = jnp.concatenate([-signal[..., half_dim:], signal[..., :half_dim]], axis=-1)
    return signal * cosine_tab + turned * sine_tab

def rope_tables(positions):
    inverse_freq = 1.0 / ROPE_BASE ** (jnp.arange(0, HEAD_DIM, 2).astype(jnp.float32) / HEAD_DIM)
    angles = positions.astype(jnp.float32)[:, None] * inverse_freq[None, :]
    cosine_tab = jnp.cos(angles)
    sine_tab = jnp.sin(angles)
    return (jnp.concatenate([cosine_tab, cosine_tab], axis=-1), jnp.concatenate([sine_tab, sine_tab], axis=-1))

def layer_forward(weights, signal, cosine_tab, sine_tab):
    gain_one, wqkv_mat, bqkv_vec, wout_mat, gain_two, wgate_mat, wup_mat, wdown_mat = weights
    groups = signal.shape[0]
    length = signal.shape[1]
    repeat = HEADS // KV_HEADS
    normed = low(rms_scale(signal, gain_one))
    projected = low_back(jnp.einsum('gtd,de->gte', normed, wqkv_mat, precision=HIGHEST) + bqkv_vec)
    queries = projected[..., :QDIM].reshape(groups, length, HEADS, HEAD_DIM)
    keys_pre = projected[..., QDIM:QDIM + KVDIM].reshape(groups, length, KV_HEADS, HEAD_DIM)
    values_pre = projected[..., QDIM + KVDIM:].reshape(groups, length, KV_HEADS, HEAD_DIM)
    cos_b = cosine_tab[:, None, :]
    sin_b = sine_tab[:, None, :]
    queries = low(low_back(rotate(queries, cos_b, sin_b)))
    keys_rep = low(low_back(jnp.repeat(rotate(keys_pre, cos_b, sin_b), repeat, axis=2)))
    values_rep = low(low_back(jnp.repeat(values_pre, repeat, axis=2)))
    score_scale = 1.0 / math.sqrt(HEAD_DIM)
    scores = low_back(jnp.einsum('gqhe,gkhe->ghqk', queries, keys_rep, precision=HIGHEST) * score_scale)
    positions = jnp.arange(length)
    causal = positions[:, None] >= positions[None, :]
    scores = jnp.where(causal, scores, MASK_LOW)
    chances = low(jax.nn.softmax(scores, axis=-1))
    attended = jnp.einsum('ghqk,gkhe->gqhe', chances, values_rep, precision=HIGHEST)
    attended = low(low_back(attended)).reshape(groups, length, QDIM)
    branch = low_back(jnp.einsum('gtd,de->gte', attended, wout_mat, precision=HIGHEST))
    middle = signal + branch
    normed_two = low(rms_scale(middle, gain_two))
    gate_pre = low_back(jnp.einsum('gtd,df->gtf', normed_two, wgate_mat, precision=HIGHEST))
    up_proj = low_back(jnp.einsum('gtd,df->gtf', normed_two, wup_mat, precision=HIGHEST))
    activated = low(jax.nn.silu(gate_pre) * up_proj)
    mlp_out = low_back(jnp.einsum('gtf,fd->gtd', activated, wdown_mat, precision=HIGHEST))
    return middle + mlp_out

def reference(inputs, gain_attn, w_qkv, b_qkv, w_out, gain_mlp, w_gate, w_up, w_down, cotangent):
    params = tuple((member.astype(jnp.float32) for member in (gain_attn, w_qkv, b_qkv, w_out, gain_mlp, w_gate, w_up, w_down)))
    length = SEQ_LEN
    per_step = max(1, min(N_DP, 4096 // length))
    step_count = N_DP // per_step
    seq_inputs = inputs.astype(jnp.float32).reshape(step_count, per_step, length, D)
    seq_cot = cotangent.astype(jnp.float32).reshape(step_count, per_step, length, D)
    cosine_tab, sine_tab = rope_tables(jnp.arange(length, dtype=jnp.int32))

    def one_step(running, paired):
        batch_in, batch_cot = paired
        result, pullback = jax.vjp(lambda weights, signal: layer_forward(weights, signal, cosine_tab, sine_tab), params, batch_in)
        grad_params, grad_in = pullback(batch_cot)
        running = jax.tree.map(lambda summed, added: summed + added, running, grad_params)
        return (running, (result.astype(jnp.bfloat16), grad_in))
    start_grads = jax.tree.map(jnp.zeros_like, params)
    totals, (outputs, grad_all) = lax.scan(one_step, start_grads, (seq_inputs, seq_cot))
    return (outputs.reshape(TOKENS, D), grad_all.reshape(TOKENS, D), totals[0], totals[1], totals[2], totals[3], totals[4], totals[5], totals[6], totals[7])
```

```python
import math

import jax
import jax.numpy as jnp
from jax import lax
from jax.experimental import pallas as pl
from jax.experimental.pallas import tpu as pltpu
from jax.sharding import PartitionSpec as P

HEADS = 16
KV_HEADS = 16
HEAD_DIM = 64


NORM_EPS = 1e-06
ROPE_BASE = 1000000.0
MASK_LOW = -1000000000.0


def rms_scale(signal, gain_vec):
    return (
        signal * lax.rsqrt(jnp.mean(signal * signal, axis=-1, keepdims=True) + NORM_EPS) * gain_vec
    )


def rotate(signal, cosine_tab, sine_tab):
    half_dim = signal.shape[-1] // 2
    turned = jnp.concatenate([-signal[..., half_dim:], signal[..., :half_dim]], axis=-1)
    return signal * cosine_tab + turned * sine_tab


def unrotate(grad_in, cosine_tab, sine_tab):
    half_dim = grad_in.shape[-1] // 2
    shifted = grad_in * sine_tab
    flipped = jnp.concatenate([shifted[..., half_dim:], -shifted[..., :half_dim]], axis=-1)
    return grad_in * cosine_tab + flipped


def rope_tables(positions):
    inverse_freq = 1.0 / ROPE_BASE ** (jnp.arange(0, HEAD_DIM, 2).astype(jnp.float32) / HEAD_DIM)
    angles = positions.astype(jnp.float32)[:, None] * inverse_freq[None, :]
    cosine_tab = jnp.cos(angles)
    sine_tab = jnp.sin(angles)
    return (
        jnp.concatenate([cosine_tab, cosine_tab], axis=-1),
        jnp.concatenate([sine_tab, sine_tab], axis=-1),
    )


def times_trans(left_op, weight):
    return lax.dot_general(
        left_op, weight, (((1,), (1,)), ((), ())), preferred_element_type=jnp.float32
    )


def trans_times(left_op, right_op):
    return lax.dot_general(
        left_op, right_op, (((0,), (0,)), ((), ())), preferred_element_type=jnp.float32
    )


def masked_scores(query_rows, keys_all, block_index, block_len):
    length = keys_all.shape[0]
    score_scale = 1.0 / math.sqrt(HEAD_DIM)
    scores = (
        jnp.einsum("qhe,khe->hqk", query_rows, keys_all, preferred_element_type=jnp.float32)
        * score_scale
    )
    query_pos = block_index * block_len + jnp.arange(block_len)
    key_pos = jnp.arange(length)
    return jnp.where(query_pos[:, None] >= key_pos[None, :], scores, MASK_LOW)


def attend_forward(queries, keys_all, values_all):
    length = queries.shape[0]
    block_len = min(512, length)
    block_count = length // block_len

    def one_block(block_index):
        scores = masked_scores(queries, keys_all, block_index, block_len)
        row_top = jnp.max(scores, axis=-1, keepdims=True)
        lifted = jnp.exp(scores - row_top)
        row_total = jnp.sum(lifted, axis=-1, keepdims=True)
        chances = (lifted / row_total).astype(jnp.bfloat16)
        block_out = jnp.einsum(
            "hqk,khe->qhe", chances, values_all, preferred_element_type=jnp.float32
        ).astype(jnp.bfloat16)
        log_total = (row_top + jnp.log(row_total))[..., 0]
        return (block_out, log_total)

    outs_all, log_totals = lax.map(one_block, jnp.arange(block_count))
    return (outs_all.reshape(queries.shape), log_totals)


def attend_backward(queries, keys_all, values_all, log_totals, grad_rows_all):
    length = queries.shape[0]
    block_len = min(512, length)
    block_count = length // block_len
    score_scale = 1.0 / math.sqrt(HEAD_DIM)

    def one_block(running, block_index):
        grad_keys, grad_values = running
        scores = masked_scores(queries, keys_all, block_index, block_len)
        log_total = lax.dynamic_index_in_dim(log_totals, block_index, 0, keepdims=False)
        chances = jnp.exp(scores - log_total[..., None])
        chances_low = chances.astype(jnp.bfloat16)
        grad_values = grad_values + jnp.einsum(
            "hqk,qhe->khe", chances_low, grad_rows_all, preferred_element_type=jnp.float32
        )
        grad_chances = jnp.einsum(
            "qhe,khe->hqk", grad_rows_all, values_all, preferred_element_type=jnp.float32
        )
        inner_sum = jnp.sum(chances * grad_chances, axis=-1, keepdims=True)
        grad_scores = (chances * (grad_chances - inner_sum)).astype(jnp.bfloat16)
        grad_query = (
            jnp.einsum("hqk,khe->qhe", grad_scores, keys_all, preferred_element_type=jnp.float32)
            * score_scale
        ).astype(jnp.bfloat16)
        grad_keys = (
            grad_keys
            + jnp.einsum("hqk,qhe->khe", grad_scores, queries, preferred_element_type=jnp.float32)
            * score_scale
        )
        return ((grad_keys, grad_values), grad_query)

    zeros_kv = jnp.zeros(keys_all.shape, jnp.float32)
    (grad_keys, grad_values), grad_queries = lax.scan(
        one_block, (zeros_kv, zeros_kv), jnp.arange(block_count)
    )
    return (
        grad_queries.reshape(queries.shape),
        grad_keys.astype(jnp.bfloat16),
        grad_values.astype(jnp.bfloat16),
    )


def generic_body(inputs, gain_attn, w_qkv, b_qkv, w_out, gain_mlp, w_gate, w_up, w_down, cotangent):
    tokens = inputs.shape[0]
    repeat = HEADS // KV_HEADS
    q_width = HEADS * HEAD_DIM
    kv_width = KV_HEADS * HEAD_DIM
    ff_width = w_gate.shape[1]
    attn_set = (
        lax.all_gather(gain_attn, "dp", axis=0, tiled=True),
        lax.all_gather(w_qkv, "dp", axis=0, tiled=True),
        lax.all_gather(b_qkv, "dp", axis=0, tiled=True),
        lax.all_gather(w_out, "dp", axis=0, tiled=True),
    )
    mlp_set = (
        lax.all_gather(gain_mlp, "dp", axis=0, tiled=True),
        lax.all_gather(w_gate, "dp", axis=0, tiled=True),
        lax.all_gather(w_up, "dp", axis=0, tiled=True),
        lax.all_gather(w_down, "dp", axis=0, tiled=True),
    )
    gain_one, wqkv_full, bqkv_full, wout_full = attn_set
    gain_two, wgate_full, wup_full, wdown_full = mlp_set
    hidden_in = inputs.astype(jnp.float32)
    positions = lax.axis_index("seq") * tokens + jnp.arange(tokens, dtype=jnp.int32)
    cosine_tab, sine_tab = rope_tables(positions)
    cos_b = cosine_tab[:, None, :]
    sin_b = sine_tab[:, None, :]
    normed, norm_pull = jax.vjp(rms_scale, hidden_in, gain_one.astype(jnp.float32))
    normed_low = normed.astype(jnp.bfloat16)
    projected = jnp.dot(
        normed_low, wqkv_full, preferred_element_type=jnp.float32
    ) + bqkv_full.astype(jnp.float32)
    queries = projected[:, :q_width].reshape(tokens, HEADS, HEAD_DIM)
    keys_pre = projected[:, q_width : q_width + kv_width].reshape(tokens, KV_HEADS, HEAD_DIM)
    values_pre = projected[:, q_width + kv_width :].reshape(tokens, KV_HEADS, HEAD_DIM)
    queries_low = rotate(queries, cos_b, sin_b).astype(jnp.bfloat16)
    keys_low = jnp.repeat(rotate(keys_pre, cos_b, sin_b), repeat, axis=1).astype(jnp.bfloat16)
    values_low = jnp.repeat(values_pre, repeat, axis=1).astype(jnp.bfloat16)
    query_heads, key_heads, value_heads = (
        lax.all_to_all(queries_low, "seq", split_axis=1, concat_axis=0, tiled=True),
        lax.all_to_all(keys_low, "seq", split_axis=1, concat_axis=0, tiled=True),
        lax.all_to_all(values_low, "seq", split_axis=1, concat_axis=0, tiled=True),
    )
    attended, log_totals = attend_forward(query_heads, key_heads, value_heads)
    attended_tok = lax.all_to_all(attended, "seq", split_axis=0, concat_axis=1, tiled=True)
    attended_flat = attended_tok.reshape(tokens, q_width)
    middle = hidden_in + jnp.dot(attended_flat, wout_full, preferred_element_type=jnp.float32)
    normed_two, norm_two_pull = jax.vjp(rms_scale, middle, gain_two.astype(jnp.float32))
    normed_two_low = normed_two.astype(jnp.bfloat16)
    gate_pre = jnp.dot(normed_two_low, wgate_full, preferred_element_type=jnp.float32)
    up_proj = jnp.dot(normed_two_low, wup_full, preferred_element_type=jnp.float32)
    activated, act_pull = jax.vjp(
        lambda gate_in, up_in: jax.nn.silu(gate_in) * up_in, gate_pre, up_proj
    )
    activated_low = activated.astype(jnp.bfloat16)
    mlp_out = jnp.dot(activated_low, wdown_full, preferred_element_type=jnp.float32)
    output = (middle + mlp_out).astype(jnp.bfloat16)
    attn_back = (
        lax.all_gather(gain_attn, "dp", axis=0, tiled=True),
        lax.all_gather(w_qkv, "dp", axis=0, tiled=True),
        lax.all_gather(b_qkv, "dp", axis=0, tiled=True),
        lax.all_gather(w_out, "dp", axis=0, tiled=True),
    )
    mlp_back = (
        lax.all_gather(gain_mlp, "dp", axis=0, tiled=True),
        lax.all_gather(w_gate, "dp", axis=0, tiled=True),
        lax.all_gather(w_up, "dp", axis=0, tiled=True),
        lax.all_gather(w_down, "dp", axis=0, tiled=True),
    )
    wqkv_back = attn_back[1]
    wout_back = attn_back[3]
    wgate_back = mlp_back[1]
    wup_back = mlp_back[2]
    wdown_back = mlp_back[3]
    grad_out = cotangent.astype(jnp.float32)
    grad_act = times_trans(cotangent, wdown_back)
    grad_gate, grad_up = act_pull(grad_act)
    grad_gate_low = grad_gate.astype(jnp.bfloat16)
    grad_up_low = grad_up.astype(jnp.bfloat16)
    grad_normed_two = times_trans(grad_gate_low, wgate_back) + times_trans(grad_up_low, wup_back)
    grad_middle_norm, grad_gain_two = norm_two_pull(grad_normed_two)
    grad_middle = grad_out + grad_middle_norm
    grad_middle_low = grad_middle.astype(jnp.bfloat16)
    grad_attended = times_trans(grad_middle_low, wout_back).astype(jnp.bfloat16)
    grad_heads_in = lax.all_to_all(
        grad_attended.reshape(tokens, HEADS, HEAD_DIM),
        "seq",
        split_axis=1,
        concat_axis=0,
        tiled=True,
    )
    grad_q, grad_k, grad_v = attend_backward(
        query_heads, key_heads, value_heads, log_totals, grad_heads_in
    )
    grad_q_tok, grad_k_tok, grad_v_tok = (
        lax.all_to_all(grad_q, "seq", split_axis=0, concat_axis=1, tiled=True),
        lax.all_to_all(grad_k, "seq", split_axis=0, concat_axis=1, tiled=True),
        lax.all_to_all(grad_v, "seq", split_axis=0, concat_axis=1, tiled=True),
    )
    grad_k_sum = jnp.sum(
        grad_k_tok.astype(jnp.float32).reshape(tokens, KV_HEADS, repeat, HEAD_DIM), axis=2
    )
    grad_v_sum = jnp.sum(
        grad_v_tok.astype(jnp.float32).reshape(tokens, KV_HEADS, repeat, HEAD_DIM), axis=2
    )
    grad_q_pre = unrotate(grad_q_tok.astype(jnp.float32), cos_b, sin_b)
    grad_k_pre = unrotate(grad_k_sum, cos_b, sin_b)
    grad_proj = jnp.concatenate(
        [
            grad_q_pre.reshape(tokens, q_width),
            grad_k_pre.reshape(tokens, kv_width),
            grad_v_sum.reshape(tokens, kv_width),
        ],
        axis=1,
    ).astype(jnp.bfloat16)
    grad_normed = times_trans(grad_proj, wqkv_back)
    grad_hidden_norm, grad_gain_one = norm_pull(grad_normed)
    grad_inputs = grad_middle + grad_hidden_norm
    term_wqkv = trans_times(normed_low, grad_proj)
    term_bqkv = jnp.sum(grad_proj.astype(jnp.float32), axis=0)
    term_wout = trans_times(attended_flat, grad_middle_low)
    sum_gain_one, sum_wqkv, sum_bqkv, sum_wout, sum_gain_two = (
        lax.psum_scatter(
            grad_gain_one.astype(jnp.bfloat16), "dp", scatter_dimension=0, tiled=True
        ).astype(jnp.float32),
        lax.psum_scatter(
            term_wqkv.astype(jnp.bfloat16), "dp", scatter_dimension=0, tiled=True
        ).astype(jnp.float32),
        lax.psum_scatter(
            term_bqkv.astype(jnp.bfloat16), "dp", scatter_dimension=0, tiled=True
        ).astype(jnp.float32),
        lax.psum_scatter(
            term_wout.astype(jnp.bfloat16), "dp", scatter_dimension=0, tiled=True
        ).astype(jnp.float32),
        lax.psum_scatter(
            grad_gain_two.astype(jnp.bfloat16), "dp", scatter_dimension=0, tiled=True
        ).astype(jnp.float32),
    )
    gate_up_low = jnp.concatenate([grad_gate_low, grad_up_low], axis=1)
    columns = normed_two_low
    sum_gate_up = lax.psum_scatter(
        trans_times(columns, gate_up_low).astype(jnp.bfloat16),
        "dp",
        scatter_dimension=0,
        tiled=True,
    )
    columns = activated_low
    sum_down = lax.psum_scatter(
        trans_times(columns, cotangent).astype(jnp.bfloat16), "dp", scatter_dimension=0, tiled=True
    )
    totals = (
        lax.psum(sum_gain_one.astype(jnp.bfloat16), "seq").astype(jnp.float32),
        lax.psum(sum_wqkv.astype(jnp.bfloat16), "seq").astype(jnp.float32),
        lax.psum(sum_bqkv.astype(jnp.bfloat16), "seq").astype(jnp.float32),
        lax.psum(sum_wout.astype(jnp.bfloat16), "seq").astype(jnp.float32),
        lax.psum(sum_gain_two.astype(jnp.bfloat16), "seq").astype(jnp.float32),
        lax.psum(sum_gate_up, "seq").astype(jnp.float32),
        lax.psum(sum_down, "seq").astype(jnp.float32),
    )
    grad_gate_up = totals[5]
    return (
        output,
        grad_inputs,
        totals[0],
        totals[1],
        totals[2],
        totals[3],
        totals[4],
        grad_gate_up[:, :ff_width],
        grad_gate_up[:, ff_width:],
        totals[6],
    )


Z_LEN = 4
X_LEN = 2
SEQ_PARTS = 4
MESH = pl.DeviceIdType.MESH
HBM = pl.BlockSpec(memory_space=pl.ANY)
VMEM = pl.BlockSpec(memory_space=pltpu.VMEM)
BF16 = jnp.bfloat16
F32 = jnp.float32


def place():
    dp = lax.axis_index("dp")
    part = lax.axis_index("seq")
    z, x = lax.div(dp, X_LEN), lax.rem(dp, X_LEN)
    return dp, part, z, x


def quarter_of(part):
    y, core = lax.div(part, 2), lax.rem(part, 2)
    return (1 - y) * 3 * core + y * (1 + core)


def turn(value, step, length):
    return lax.rem(value + step, length)


def remote(source, target, send, recv, dp, part):
    return pltpu.make_async_remote_copy(
        src_ref=source,
        dst_ref=target,
        send_sem=send,
        recv_sem=recv,
        device_id=(dp, part),
        device_id_type=MESH,
    )


def block(index, size):
    return pl.ds(pl.multiple_of(index * size, size), size)


def greet(partners):
    barrier = pltpu.get_barrier_semaphore()
    for dp, part in partners:
        pl.semaphore_signal(barrier, inc=1, device_id=(dp, part), device_id_type=MESH)
    pl.semaphore_wait(barrier, len(partners))


def z_partners(dp, part, z, x):
    return [(turn(z, step, Z_LEN) * X_LEN + x, part) for step in range(1, Z_LEN)]


def seq_partners(dp, part):
    return [(dp, turn(part, step, SEQ_PARTS)) for step in range(1, SEQ_PARTS)]


class ColumnGather:
    def __init__(self, source, dest, send, recv, local, base):
        self.source, self.dest, self.send, self.recv, self.local, self.base = (
            source, dest, send, recv, local, base,
        )
        self.rows = dest.shape[0] // (Z_LEN * X_LEN)

    def slot(self, dp):
        return self.dest.at[block(dp, self.rows)]

    def copy(self, source, slot, index, dp, part):
        return remote(
            source, slot, self.send.at[self.base + index], self.recv.at[self.base + index], dp, part
        )

    def start(self):
        dp, part, z, x = place()
        mine = self.slot(dp)
        self.own = pltpu.make_async_copy(self.source, mine, self.local)
        self.own.start()
        self.sent = []
        for step in range(1, Z_LEN):
            self.sent.append(
                self.copy(self.source, mine, step - 1, turn(z, step, Z_LEN) * X_LEN + x, part)
            )
        self.sent.append(self.copy(self.source, mine, 3, z * X_LEN + 1 - x, part))
        for each in self.sent:
            each.start()

    def relay(self):
        dp, part, z, x = place()
        for step in range(1, Z_LEN):
            slot = self.slot(turn(z, Z_LEN - step, Z_LEN) * X_LEN + x)
            self.copy(slot, slot, step - 1, dp, part).wait_recv()
            onward = self.copy(slot, slot, 3 + step, z * X_LEN + 1 - x, part)
            onward.start()
            self.sent.append(onward)

    def arrive(self):
        dp, part, z, x = place()
        self.own.wait()
        for step in range(Z_LEN):
            slot = self.slot(turn(z, Z_LEN - step, Z_LEN) * X_LEN + 1 - x)
            self.copy(slot, slot, 3 + step, dp, part).wait_recv()

    def drain(self):
        for each in self.sent:
            each.wait_send()


class RowGather:
    def __init__(self, source, dest, send, recv, local, base):
        self.source, self.dest, self.send, self.recv, self.local, self.base = (
            source, dest, send, recv, local, base,
        )
        self.rows = dest.shape[0] // X_LEN

    def slot(self, x):
        return self.dest.at[block(x, self.rows)]

    def copy(self, source, slot, send, recv, dp, part):
        return remote(
            source, slot, self.send.at[self.base + send], self.recv.at[self.base + recv], dp, part
        )

    def start(self):
        dp, part, z, x = place()
        quarter = quarter_of(part)
        mine = self.slot(x)

        @pl.when(z == quarter)
        def _():
            pltpu.make_async_copy(self.source, mine, self.local).start()
            for step in range(1, Z_LEN):
                self.copy(
                    self.source, mine, step - 1, 0, turn(z, step, Z_LEN) * X_LEN + x, part
                ).start()
            self.copy(self.source, mine, 3, 1, z * X_LEN + 1 - x, part).start()

    def relay(self):
        dp, part, z, x = place()
        mine = self.slot(x)

        @pl.when(z != quarter_of(part))
        def _():
            self.copy(mine, mine, 0, 0, dp, part).wait_recv()
            self.copy(mine, mine, 3, 1, z * X_LEN + 1 - x, part).start()

    def arrive(self):
        dp, part, z, x = place()
        mine, other = self.slot(x), self.slot(1 - x)

        @pl.when(z == quarter_of(part))
        def _():
            pltpu.make_async_copy(self.source, mine, self.local).wait()

        self.copy(other, other, 3, 1, dp, part).wait_recv()

    def drain(self):
        dp, part, z, x = place()
        mine = self.slot(x)

        @pl.when(z == quarter_of(part))
        def _():
            for step in range(1, Z_LEN):
                self.copy(self.source, mine, step - 1, 0, dp, part).wait_send()

        self.copy(self.source, mine, 3, 1, dp, part).wait_send()


class SeqGather:
    def __init__(self, source, dest, send, recv, local, base):
        self.source, self.dest, self.send, self.recv, self.local, self.base = (
            source, dest, send, recv, local, base,
        )
        self.rows = dest.shape[0] // SEQ_PARTS

    def copy(self, slot, index, dp, part):
        return remote(
            self.source,
            self.dest.at[block(slot, self.rows)],
            self.send.at[self.base + index],
            self.recv.at[self.base + index],
            dp,
            part,
        )

    def start(self):
        dp, part, z, x = place()
        self.own = pltpu.make_async_copy(
            self.source, self.dest.at[block(part, self.rows)], self.local
        )
        self.own.start()
        for step in range(1, SEQ_PARTS):
            self.copy(part, step - 1, dp, turn(part, step, SEQ_PARTS)).start()

    def arrive(self):
        dp, part, z, x = place()
        self.own.wait()
        for step in range(1, SEQ_PARTS):
            self.copy(turn(part, SEQ_PARTS - step, SEQ_PARTS), step - 1, dp, part).wait_recv()

    def drain(self):
        dp, part, z, x = place()
        for step in range(1, SEQ_PARTS):
            self.copy(part, step - 1, dp, part).wait_send()


def gather_kernel(
    x_in, cot, small, qkv, wout, gate_up, wdown,
    x_all, cot_all, small_all, qkv_all, wout_all, gate_up_all, wdown_all,
    send, recv, local,
):
    dp, part, z, x = place()
    greet(
        z_partners(dp, part, z, x)
        + [(z * X_LEN + 1 - x, part)]
        + seq_partners(dp, part)
    )
    seq_moves = [
        SeqGather(x_in, x_all, send, recv, local.at[0], 0),
        SeqGather(cot, cot_all, send, recv, local.at[1], 3),
    ]
    moves = [
        ColumnGather(small, small_all, send, recv, local.at[2], 8),
        ColumnGather(qkv, qkv_all, send, recv, local.at[3], 16),
        RowGather(wout, wout_all, send, recv, local.at[4], 24),
        ColumnGather(gate_up, gate_up_all, send, recv, local.at[5], 32),
        RowGather(wdown, wdown_all, send, recv, local.at[6], 40),
    ]
    for move in seq_moves + moves:
        move.start()
    for move in moves:
        move.relay()
    for move in seq_moves + moves:
        move.arrive()
    for move in seq_moves + moves:
        move.drain()


def gather_all(x_in, cot, small, qkv, wout, gate_up, wdown):
    def grown(array, times):
        return jax.ShapeDtypeStruct((array.shape[0] * times,) + array.shape[1:], array.dtype)

    dp = Z_LEN * X_LEN
    return pl.pallas_call(
        gather_kernel,
        out_shape=(
            grown(x_in, SEQ_PARTS), grown(cot, SEQ_PARTS), grown(small, dp), grown(qkv, dp),
            grown(wout, X_LEN), grown(gate_up, dp), grown(wdown, X_LEN),
        ),
        in_specs=[HBM] * 7,
        out_specs=[VMEM] * 7,
        scratch_shapes=[
            pltpu.SemaphoreType.DMA((48,)),
            pltpu.SemaphoreType.DMA((48,)),
            pltpu.SemaphoreType.DMA((8,)),
        ],
        compiler_params=pltpu.CompilerParams(collective_id=0, has_side_effects=True),
    )(x_in, cot, small, qkv, wout, gate_up, wdown)


def over_rows(count, step, work):
    def one(index, carry):
        work(pl.ds(pl.multiple_of(index * step, step), step))
        return carry

    lax.fori_loop(0, count // step, one, 0)


def mean_square(value):
    return lax.rsqrt(jnp.mean(value * value, axis=-1, keepdims=True) + NORM_EPS)


class SeqReduce:
    def __init__(self, partial, outbox, inbox, send, recv, base):
        self.partial, self.outbox, self.inbox, self.send, self.recv, self.base = (
            partial, outbox, inbox, send, recv, base,
        )
        self.rows = partial.shape[0] // SEQ_PARTS

    def copy(self, index, dp, part):
        return remote(
            self.outbox.at[index],
            self.inbox.at[index],
            self.send.at[self.base + index],
            self.recv.at[self.base + index],
            dp,
            part,
        )

    def start(self):
        dp, part, z, x = place()
        for step in range(1, SEQ_PARTS):
            target = turn(part, step, SEQ_PARTS)

            def work(rows, target=target, step=step):
                self.outbox[step - 1, rows, :] = self.partial[
                    pl.ds(pl.multiple_of(target * self.rows + rows.start, rows.size), rows.size), :
                ].astype(BF16)

            over_rows(self.rows, 16, work)
            self.copy(step - 1, dp, target).start()

    def arrive(self):
        dp, part, z, x = place()
        for step in range(1, SEQ_PARTS):
            self.copy(step - 1, dp, part).wait_recv()

    def total(self, rows):
        dp, part, z, x = place()
        value = self.partial[
            pl.ds(pl.multiple_of(part * self.rows + rows.start, rows.size), rows.size), :
        ]
        for step in range(SEQ_PARTS - 1):
            value = value + self.inbox[step, rows, :].astype(F32)
        return value

    def drain(self):
        dp, part, z, x = place()
        for step in range(1, SEQ_PARTS):
            self.copy(step - 1, dp, part).wait_send()


def middle_kernel(partial, x_in, gain, mid, normed_all, normed, outbox, inbox, send, recv, local):
    dp, part, z, x = place()
    greet(seq_partners(dp, part))
    reduce = SeqReduce(partial, outbox, inbox, send, recv, 0)
    reduce.start()
    reduce.arrive()

    def work(rows):
        value = x_in[rows, :].astype(F32) + reduce.total(rows)
        mid[rows, :] = value
        normed[rows, :] = (value * mean_square(value) * gain[...]).astype(BF16)

    over_rows(x_in.shape[0], 16, work)
    spread = SeqGather(normed, normed_all, send, recv, local.at[0], 3)
    spread.start()
    spread.arrive()
    reduce.drain()
    spread.drain()


def seq_scratch(rows, width):
    return [
        pltpu.VMEM((rows, width), BF16),
        pltpu.VMEM((SEQ_PARTS - 1, rows, width), BF16),
        pltpu.VMEM((SEQ_PARTS - 1, rows, width), BF16),
        pltpu.SemaphoreType.DMA((8,)),
        pltpu.SemaphoreType.DMA((8,)),
        pltpu.SemaphoreType.DMA((1,)),
    ]


def middle_step(partial, x_in, gain):
    rows, width = x_in.shape
    return pl.pallas_call(
        middle_kernel,
        out_shape=(
            jax.ShapeDtypeStruct((rows, width), F32),
            jax.ShapeDtypeStruct((rows * SEQ_PARTS, width), BF16),
        ),
        in_specs=[VMEM] * 3,
        out_specs=[VMEM] * 2,
        scratch_shapes=seq_scratch(rows, width),
        compiler_params=pltpu.CompilerParams(collective_id=1, has_side_effects=True),
    )(partial, x_in, gain)


def rms_back(value, grad, gain):
    scale = mean_square(value)
    unit = value * scale
    pulled = grad * gain
    inner = jnp.mean(pulled * unit, axis=-1, keepdims=True)
    return scale * (pulled - unit * inner), grad * unit


def back_kernel(
    partial, mid, base, gain, grad_mid, low_all, grad_gain, low, outbox, inbox, send, recv, local
):
    dp, part, z, x = place()
    greet(seq_partners(dp, part))
    reduce = SeqReduce(partial, outbox, inbox, send, recv, 0)
    reduce.start()
    grad_gain[...] = jnp.zeros_like(grad_gain)
    reduce.arrive()

    def work(rows):
        pulled, summand = rms_back(mid[rows, :], reduce.total(rows), gain[...])
        total = base[rows, :].astype(F32) + pulled
        grad_mid[rows, :] = total
        low[rows, :] = total.astype(BF16)
        grad_gain[...] += jnp.sum(summand, axis=0, keepdims=True)

    over_rows(mid.shape[0], 16, work)
    spread = SeqGather(low, low_all, send, recv, local.at[0], 3)
    spread.start()
    spread.arrive()
    reduce.drain()
    spread.drain()


def back_step(partial, mid, base, gain, number):
    rows, width = mid.shape
    return pl.pallas_call(
        back_kernel,
        out_shape=(
            jax.ShapeDtypeStruct((rows, width), F32),
            jax.ShapeDtypeStruct((rows * SEQ_PARTS, width), BF16),
            jax.ShapeDtypeStruct((1, width), F32),
        ),
        in_specs=[VMEM] * 4,
        out_specs=[VMEM] * 3,
        scratch_shapes=seq_scratch(rows, width),
        compiler_params=pltpu.CompilerParams(collective_id=number, has_side_effects=True),
    )(partial, mid, base, gain)


class ColumnReduce:
    def __init__(self, grads, xbox, hold, zbox, out, send, recv, base):
        self.grads, self.xbox, self.hold, self.zbox, self.out = grads, xbox, hold, zbox, out
        self.send, self.recv, self.base = send, recv, base
        self.rows = grads.shape[0] // (Z_LEN * X_LEN)

    def copy(self, source, slot, index, dp, part):
        return remote(
            source, slot, self.send.at[self.base + index], self.recv.at[self.base + index], dp, part
        )

    def order(self):
        return range(Z_LEN - 1, -1, -1)

    def cross(self, step):
        dp, part, z, x = place()
        target = turn(z, step, Z_LEN)
        return self.copy(
            self.grads.at[block(target * X_LEN + 1 - x, self.rows)],
            self.xbox.at[step],
            step,
            z * X_LEN + 1 - x,
            part,
        )

    def along(self, step):
        dp, part, z, x = place()
        return self.copy(
            self.hold.at[step],
            self.zbox.at[step],
            3 + step,
            turn(z, step, Z_LEN) * X_LEN + x,
            part,
        )

    def share(self, step):
        dp, part, z, x = place()
        return self.copy(
            self.out.at[part], self.out.at[part], 6 + step, dp, turn(part, step, SEQ_PARTS)
        )

    def start(self):
        for step in self.order():
            self.cross(step).start()

    def relay(self):
        dp, part, z, x = place()
        for step in self.order():
            self.cross(step).wait_recv()
            mine = turn(z, step, Z_LEN) * X_LEN + x

            def work(rows, step=step, mine=mine):
                here = pl.ds(pl.multiple_of(mine * self.rows + rows.start, 16), 16)
                self.hold[step, rows, :] = (
                    self.grads[here, :].astype(F32) + self.xbox[step, rows, :].astype(F32)
                ).astype(BF16)

            over_rows(self.rows, 16, work)
            if step:
                self.along(step).start()

    def finish(self):
        dp, part, z, x = place()
        for step in range(1, Z_LEN):
            self.along(step).wait_recv()

        def work(rows):
            value = self.hold[0, rows, :].astype(F32)
            for step in range(1, Z_LEN):
                value = value + self.zbox[step, rows, :].astype(F32)
            self.out[part, rows, :] = value.astype(BF16)

        over_rows(self.rows, 16, work)
        for step in range(1, SEQ_PARTS):
            self.share(step).start()

    def drain(self):
        dp, part, z, x = place()
        for step in range(1, SEQ_PARTS):
            slot = self.out.at[turn(part, SEQ_PARTS - step, SEQ_PARTS)]
            self.copy(slot, slot, 6 + step, dp, part).wait_recv()
            self.share(step).wait_send()
            self.along(step).wait_send()
        for step in self.order():
            self.cross(step).wait_send()


class RowReduce:
    def __init__(self, grads, xbox, hold, zbox, out, send, recv, base):
        self.grads, self.xbox, self.hold, self.zbox, self.out = grads, xbox, hold, zbox, out
        self.send, self.recv, self.base = send, recv, base
        self.rows = grads.shape[0] // X_LEN

    def copy(self, source, slot, send, recv, dp, part):
        return remote(
            source, slot, self.send.at[self.base + send], self.recv.at[self.base + recv], dp, part
        )

    def cross(self):
        dp, part, z, x = place()
        return self.copy(
            self.grads.at[block(1 - x, self.rows)], self.xbox, 0, 0, z * X_LEN + 1 - x, part
        )

    def along(self, step):
        dp, part, z, x = place()
        return self.copy(
            self.hold, self.zbox.at[step], 1, 1 + step, quarter_of(part) * X_LEN + x, part
        )

    def share(self, step, source_part):
        dp, part, z, x = place()
        return self.copy(
            self.out, self.out, 1 + step, 5, dp, turn(source_part, step, SEQ_PARTS)
        )

    def start(self):
        self.cross().start()

    def relay(self):
        dp, part, z, x = place()
        self.cross().wait_recv()

        def work(rows):
            here = pl.ds(pl.multiple_of(x * self.rows + rows.start, 16), 16)
            self.hold[rows, :] = (
                self.grads[here, :].astype(F32) + self.xbox[rows, :].astype(F32)
            ).astype(BF16)

        over_rows(self.rows, 16, work)
        gap = turn(quarter_of(part), Z_LEN - z, Z_LEN)
        for step in range(1, Z_LEN):

            @pl.when(gap == step)
            def _(step=step):
                self.along(step).start()

    def finish(self):
        dp, part, z, x = place()

        @pl.when(z == quarter_of(part))
        def _():
            for step in range(1, Z_LEN):
                self.along(step).wait_recv()

            def work(rows):
                value = self.hold[rows, :].astype(F32)
                for step in range(1, Z_LEN):
                    value = value + self.zbox[step, rows, :].astype(F32)
                self.out[rows, :] = value.astype(BF16)

            over_rows(self.rows, 16, work)
            for step in range(1, SEQ_PARTS):
                self.share(step, part).start()

    def drain(self):
        dp, part, z, x = place()
        self.cross().wait_send()

        @pl.when(z == quarter_of(part))
        def _():
            for step in range(1, SEQ_PARTS):
                self.share(step, part).wait_send()

        @pl.when(z != quarter_of(part))
        def _():
            self.along(1).wait_send()
            self.copy(self.out, self.out, 1, 5, dp, part).wait_recv()


class VectorReduce:
    def __init__(self, vector, seq_box, dp_box, out, send, recv, base):
        self.vector, self.seq_box, self.dp_box, self.out = vector, seq_box, dp_box, out
        self.send, self.recv, self.base = send, recv, base
        self.rows = vector.shape[0] // (Z_LEN * X_LEN)

    def copy(self, source, slot, index, dp, part):
        return remote(
            source, slot, self.send.at[self.base + index], self.recv.at[self.base + index], dp, part
        )

    def near(self, step):
        dp, part, z, x = place()
        return self.copy(
            self.seq_box.at[part], self.seq_box.at[part], step, dp, turn(part, step, SEQ_PARTS)
        )

    def far(self, step):
        dp, part, z, x = place()
        target = turn(dp, step, Z_LEN * X_LEN)
        return self.copy(
            self.vector.at[block(target, self.rows)], self.dp_box.at[dp], 4 + step, target, part
        )

    def start(self):
        dp, part, z, x = place()
        self.seq_box[part] = self.vector[...]
        for step in range(1, SEQ_PARTS):
            self.near(step).start()

    def relay(self):
        dp, part, z, x = place()
        for step in range(1, SEQ_PARTS):
            slot = self.seq_box.at[turn(part, SEQ_PARTS - step, SEQ_PARTS)]
            self.copy(slot, slot, step, dp, part).wait_recv()
        value = self.seq_box[0]
        for step in range(1, SEQ_PARTS):
            value = value + self.seq_box[step]
        self.vector[...] = value
        self.dp_box[dp] = self.vector[block(dp, self.rows), :]
        for step in range(1, Z_LEN * X_LEN):
            self.far(step).start()

    def finish(self):
        dp, part, z, x = place()
        count = Z_LEN * X_LEN
        for step in range(1, count):
            slot = self.dp_box.at[turn(dp, count - step, count)]
            self.copy(slot, slot, 4 + step, dp, part).wait_recv()
        value = self.dp_box[0]
        for step in range(1, count):
            value = value + self.dp_box[step]
        self.out[...] = value

    def drain(self):
        for step in range(1, SEQ_PARTS):
            self.near(step).wait_send()
        for step in range(1, Z_LEN * X_LEN):
            self.far(step).wait_send()


def reduce_kernel(
    vector_in, down, gate_up, wout, qkv,
    vector_out, down_out, gate_up_out, wout_out, qkv_out,
    vector, seq_box, dp_box,
    down_x, down_h, down_z, gu_x, gu_h, gu_z, wout_x, wout_h, wout_z, qkv_x, qkv_h, qkv_z,
    send, recv,
):
    dp, part, z, x = place()
    greet(
        [(turn(dp, step, Z_LEN * X_LEN), part) for step in range(1, Z_LEN * X_LEN)]
        + seq_partners(dp, part)
    )
    vector[...] = vector_in[...]
    moves = [
        VectorReduce(vector, seq_box, dp_box, vector_out, send, recv, 0),
        RowReduce(down, down_x, down_h, down_z, down_out, send, recv, 16),
        ColumnReduce(gate_up, gu_x, gu_h, gu_z, gate_up_out, send, recv, 24),
        RowReduce(wout, wout_x, wout_h, wout_z, wout_out, send, recv, 36),
        ColumnReduce(qkv, qkv_x, qkv_h, qkv_z, qkv_out, send, recv, 44),
    ]
    for move in moves:
        move.start()
    for move in moves:
        move.relay()
    for move in moves:
        move.finish()
    for move in moves:
        move.drain()


def reduce_all(vector, down, gate_up, wout, qkv):
    def row_boxes(array):
        rows, width = array.shape[0] // X_LEN, array.shape[1]
        return [
            pltpu.VMEM((rows, width), BF16),
            pltpu.VMEM((rows, width), BF16),
            pltpu.VMEM((Z_LEN, rows, width), BF16),
        ]

    def column_boxes(array):
        rows, width = array.shape[0] // (Z_LEN * X_LEN), array.shape[1]
        return [pltpu.VMEM((Z_LEN, rows, width), BF16)] * 3

    count = Z_LEN * X_LEN
    return pl.pallas_call(
        reduce_kernel,
        out_shape=(
            jax.ShapeDtypeStruct((vector.shape[0] // count, vector.shape[1]), F32),
            jax.ShapeDtypeStruct((down.shape[0] // X_LEN, down.shape[1]), BF16),
            jax.ShapeDtypeStruct((SEQ_PARTS, gate_up.shape[0] // count, gate_up.shape[1]), BF16),
            jax.ShapeDtypeStruct((wout.shape[0] // X_LEN, wout.shape[1]), BF16),
            jax.ShapeDtypeStruct((SEQ_PARTS, qkv.shape[0] // count, qkv.shape[1]), BF16),
        ),
        in_specs=[VMEM] * 5,
        out_specs=[VMEM] * 5,
        scratch_shapes=[
            pltpu.VMEM(vector.shape, F32),
            pltpu.VMEM((SEQ_PARTS,) + vector.shape, F32),
            pltpu.VMEM((count, vector.shape[0] // count, vector.shape[1]), F32),
        ]
        + row_boxes(down)
        + column_boxes(gate_up)
        + row_boxes(wout)
        + column_boxes(qkv)
        + [pltpu.SemaphoreType.DMA((56,)), pltpu.SemaphoreType.DMA((56,))],
        compiler_params=pltpu.CompilerParams(collective_id=4, has_side_effects=True),
    )(vector, down, gate_up, wout, qkv)


def ring_body(inputs, gain_attn, w_qkv, b_qkv, w_out, gain_mlp, w_gate, w_up, w_down, cotangent):
    rows, width = inputs.shape
    count = Z_LEN * X_LEN
    part = lax.axis_index("seq")
    dp = lax.axis_index("dp")
    quarter = quarter_of(part)
    heads = HEADS // SEQ_PARTS
    inner = heads * HEAD_DIM
    ff_part = w_gate.shape[1] // SEQ_PARTS
    whole = ff_part // 128 * 128
    tokens = rows * SEQ_PARTS

    qkv_mine = lax.dynamic_index_in_dim(
        w_qkv.reshape(w_qkv.shape[0], 3, SEQ_PARTS, inner), quarter, 2, keepdims=False
    ).reshape(w_qkv.shape[0], 3 * inner)
    gate_mine = lax.dynamic_slice_in_dim(w_gate, quarter * ff_part, ff_part, 1)
    up_mine = lax.dynamic_slice_in_dim(w_up, quarter * ff_part, ff_part, 1)
    gu_mine = jnp.concatenate(
        [gate_mine[:, :whole], up_mine[:, :whole], gate_mine[:, whole:], up_mine[:, whole:]], axis=1
    )
    small = jnp.concatenate(
        [
            gain_attn.reshape(1, 128),
            gain_mlp.reshape(1, 128),
            b_qkv.reshape(3, 128),
            jnp.zeros((11, 128), BF16),
        ]
    )
    x_all, cot_all, small_all, wqkv, wout, wgu, wdown = gather_all(
        inputs, cotangent, small, qkv_mine, w_out, gu_mine, w_down
    )
    small_all = small_all.reshape(count, 16, 128).astype(F32)
    gain_one = small_all[:, 0].reshape(1, width)
    gain_two = small_all[:, 1].reshape(1, width)
    bias = lax.dynamic_index_in_dim(
        small_all[:, 2:5].reshape(3, SEQ_PARTS, inner), quarter, 1, keepdims=False
    ).reshape(1, 3 * inner)

    cosine_tab, sine_tab = rope_tables(jnp.arange(tokens, dtype=jnp.int32))
    cos_b, sin_b = cosine_tab[:, None, :], sine_tab[:, None, :]
    hidden = x_all.astype(F32)
    normed_low = rms_scale(hidden, gain_one).astype(BF16)
    projected = jnp.dot(normed_low, wqkv, preferred_element_type=F32) + bias
    pre = projected.reshape(tokens, 3, heads, HEAD_DIM)
    queries = rotate(pre[:, 0], cos_b, sin_b).astype(BF16)
    keys = rotate(pre[:, 1], cos_b, sin_b).astype(BF16)
    values = pre[:, 2].astype(BF16)
    attended, log_totals = attend_forward(queries, keys, values)
    attended_flat = attended.reshape(tokens, inner)
    mid, normed_two = middle_step(
        jnp.dot(attended_flat, wout, preferred_element_type=F32), inputs, gain_two
    )
    both = jnp.dot(normed_two, wgu, preferred_element_type=F32)
    gate = jnp.concatenate([both[:, :whole], both[:, 2 * whole : whole + ff_part]], axis=1)
    up = jnp.concatenate([both[:, whole : 2 * whole], both[:, whole + ff_part :]], axis=1)
    activated, act_pull = jax.vjp(lambda a, b: jax.nn.silu(a) * b, gate, up)
    activated_low = activated.astype(BF16)
    mlp_out = jnp.dot(activated_low, wdown, preferred_element_type=F32)
    output = (mid + lax.psum_scatter(mlp_out, "seq", scatter_dimension=0, tiled=True)).astype(BF16)

    grad_act = times_trans(cot_all, wdown)
    grad_gate, grad_up = act_pull(grad_act)
    grad_gu = jnp.concatenate(
        [grad_gate[:, :whole], grad_up[:, :whole], grad_gate[:, whole:], grad_up[:, whole:]], axis=1
    ).astype(BF16)
    grad_mid, grad_mid_all, grad_gain_two = back_step(
        times_trans(grad_gu, wgu), mid, cotangent, gain_two, 2
    )
    term_down = trans_times(activated_low, cot_all).astype(BF16)
    term_gu = trans_times(normed_two, grad_gu).astype(BF16)
    term_out = trans_times(attended_flat, grad_mid_all).astype(BF16)
    grad_attended = times_trans(grad_mid_all, wout).astype(BF16).reshape(tokens, heads, HEAD_DIM)
    grad_q, grad_k, grad_v = attend_backward(queries, keys, values, log_totals, grad_attended)
    grad_proj = jnp.stack(
        [
            unrotate(grad_q.astype(F32), cos_b, sin_b),
            unrotate(grad_k.astype(F32), cos_b, sin_b),
            grad_v.astype(F32),
        ],
        axis=1,
    ).reshape(tokens, 3 * inner).astype(BF16)
    term_qkv = trans_times(normed_low, grad_proj).astype(BF16)
    grad_inputs, _, grad_gain_one = back_step(
        times_trans(grad_proj, wqkv), inputs.astype(F32), grad_mid, gain_one, 3
    )
    bias_rows = lax.dynamic_update_slice(
        jnp.zeros((3, SEQ_PARTS, inner), F32),
        jnp.sum(grad_proj.astype(F32), axis=0).reshape(3, 1, inner),
        (0, quarter, 0),
    ).reshape(count, 3, 128)
    vector = jnp.concatenate(
        [
            grad_gain_one.reshape(count, 1, 128),
            grad_gain_two.reshape(count, 1, 128),
            bias_rows,
            jnp.zeros((count, 3, 128), F32),
        ],
        axis=1,
    ).reshape(count * 8, 128)
    sums, sum_down, sum_gu, sum_out, sum_qkv = reduce_all(
        vector, term_down, term_gu, term_out, term_qkv
    )
    order = [0, 2, 3, 1]
    parts = [sum_gu[index].astype(F32) for index in order]
    grad_w_gate = jnp.concatenate(
        [piece for each in parts for piece in (each[:, :whole], each[:, 2 * whole : whole + ff_part])],
        axis=1,
    )
    grad_w_up = jnp.concatenate(
        [piece for each in parts for piece in (each[:, whole : 2 * whole], each[:, whole + ff_part :])],
        axis=1,
    )
    grad_w_qkv = jnp.concatenate(
        [sum_qkv[index, :, kind * inner : (kind + 1) * inner] for kind in range(3) for index in order],
        axis=1,
    ).astype(F32)
    return (
        output,
        grad_inputs,
        sums[0],
        grad_w_qkv,
        sums[2:5].reshape(-1),
        sum_out.astype(F32),
        sums[1],
        grad_w_gate,
        grad_w_up,
        sum_down.astype(F32),
    )


def solution(mesh):
    tuned = mesh.shape["dp"] == Z_LEN * X_LEN and mesh.shape["seq"] == SEQ_PARTS
    return jax.shard_map(
        ring_body if tuned else generic_body,
        mesh=mesh,
        in_specs=(
            P(("dp", "seq"), None),
            P("dp"),
            P("dp", None),
            P("dp"),
            P("dp", None),
            P("dp"),
            P("dp", None),
            P("dp", None),
            P("dp", None),
            P(("dp", "seq"), None),
        ),
        out_specs=(
            P(("dp", "seq"), None),
            P(("dp", "seq"), None),
            P("dp"),
            P("dp", None),
            P("dp"),
            P("dp", None),
            P("dp"),
            P("dp", None),
            P("dp", None),
            P("dp", None),
        ),
        check_vma=False,
    )
```

```python
import math

import jax
import jax.numpy as jnp
from jax import lax
from jax.experimental import pallas as pl
from jax.experimental.pallas import tpu as pltpu
from jax.sharding import PartitionSpec as P

HEADS = 16
KV_HEADS = 16
HEAD_DIM = 64


NORM_EPS = 1e-06
ROPE_BASE = 1000000.0
MASK_LOW = -1000000000.0


def rms_scale(signal, gain_vec):
    return (
        signal * lax.rsqrt(jnp.mean(signal * signal, axis=-1, keepdims=True) + NORM_EPS) * gain_vec
    )


def rotate(signal, cosine_tab, sine_tab):
    half_dim = signal.shape[-1] // 2
    turned = jnp.concatenate([-signal[..., half_dim:], signal[..., :half_dim]], axis=-1)
    return signal * cosine_tab + turned * sine_tab


def unrotate(grad_in, cosine_tab, sine_tab):
    half_dim = grad_in.shape[-1] // 2
    shifted = grad_in * sine_tab
    flipped = jnp.concatenate([shifted[..., half_dim:], -shifted[..., :half_dim]], axis=-1)
    return grad_in * cosine_tab + flipped


def rope_tables(positions):
    inverse_freq = 1.0 / ROPE_BASE ** (jnp.arange(0, HEAD_DIM, 2).astype(jnp.float32) / HEAD_DIM)
    angles = positions.astype(jnp.float32)[:, None] * inverse_freq[None, :]
    cosine_tab = jnp.cos(angles)
    sine_tab = jnp.sin(angles)
    return (
        jnp.concatenate([cosine_tab, cosine_tab], axis=-1),
        jnp.concatenate([sine_tab, sine_tab], axis=-1),
    )


def times_trans(left_op, weight):
    return lax.dot_general(
        left_op, weight, (((1,), (1,)), ((), ())), preferred_element_type=jnp.float32
    )


def trans_times(left_op, right_op):
    return lax.dot_general(
        left_op, right_op, (((0,), (0,)), ((), ())), preferred_element_type=jnp.float32
    )


def masked_scores(query_rows, keys_all, block_index, block_len):
    length = keys_all.shape[0]
    score_scale = 1.0 / math.sqrt(HEAD_DIM)
    scores = (
        jnp.einsum("qhe,khe->hqk", query_rows, keys_all, preferred_element_type=jnp.float32)
        * score_scale
    )
    query_pos = block_index * block_len + jnp.arange(block_len)
    key_pos = jnp.arange(length)
    return jnp.where(query_pos[:, None] >= key_pos[None, :], scores, MASK_LOW)


def attend_forward(queries, keys_all, values_all):
    length = queries.shape[0]
    block_len = min(512, length)
    block_count = length // block_len

    def one_block(block_index):
        scores = masked_scores(queries, keys_all, block_index, block_len)
        row_top = jnp.max(scores, axis=-1, keepdims=True)
        lifted = jnp.exp(scores - row_top)
        row_total = jnp.sum(lifted, axis=-1, keepdims=True)
        chances = (lifted / row_total).astype(jnp.bfloat16)
        block_out = jnp.einsum(
            "hqk,khe->qhe", chances, values_all, preferred_element_type=jnp.float32
        ).astype(jnp.bfloat16)
        log_total = (row_top + jnp.log(row_total))[..., 0]
        return (block_out, log_total)

    outs_all, log_totals = lax.map(one_block, jnp.arange(block_count))
    return (outs_all.reshape(queries.shape), log_totals)


def attend_backward(queries, keys_all, values_all, log_totals, grad_rows_all):
    length = queries.shape[0]
    block_len = min(512, length)
    block_count = length // block_len
    score_scale = 1.0 / math.sqrt(HEAD_DIM)

    def one_block(running, block_index):
        grad_keys, grad_values = running
        scores = masked_scores(queries, keys_all, block_index, block_len)
        log_total = lax.dynamic_index_in_dim(log_totals, block_index, 0, keepdims=False)
        chances = jnp.exp(scores - log_total[..., None])
        chances_low = chances.astype(jnp.bfloat16)
        grad_values = grad_values + jnp.einsum(
            "hqk,qhe->khe", chances_low, grad_rows_all, preferred_element_type=jnp.float32
        )
        grad_chances = jnp.einsum(
            "qhe,khe->hqk", grad_rows_all, values_all, preferred_element_type=jnp.float32
        )
        inner_sum = jnp.sum(chances * grad_chances, axis=-1, keepdims=True)
        grad_scores = (chances * (grad_chances - inner_sum)).astype(jnp.bfloat16)
        grad_query = (
            jnp.einsum("hqk,khe->qhe", grad_scores, keys_all, preferred_element_type=jnp.float32)
            * score_scale
        ).astype(jnp.bfloat16)
        grad_keys = (
            grad_keys
            + jnp.einsum("hqk,qhe->khe", grad_scores, queries, preferred_element_type=jnp.float32)
            * score_scale
        )
        return ((grad_keys, grad_values), grad_query)

    zeros_kv = jnp.zeros(keys_all.shape, jnp.float32)
    (grad_keys, grad_values), grad_queries = lax.scan(
        one_block, (zeros_kv, zeros_kv), jnp.arange(block_count)
    )
    return (
        grad_queries.reshape(queries.shape),
        grad_keys.astype(jnp.bfloat16),
        grad_values.astype(jnp.bfloat16),
    )


def generic_body(inputs, gain_attn, w_qkv, b_qkv, w_out, gain_mlp, w_gate, w_up, w_down, cotangent):
    tokens = inputs.shape[0]
    repeat = HEADS // KV_HEADS
    q_width = HEADS * HEAD_DIM
    kv_width = KV_HEADS * HEAD_DIM
    ff_width = w_gate.shape[1]
    attn_set = (
        lax.all_gather(gain_attn, "dp", axis=0, tiled=True),
        lax.all_gather(w_qkv, "dp", axis=0, tiled=True),
        lax.all_gather(b_qkv, "dp", axis=0, tiled=True),
        lax.all_gather(w_out, "dp", axis=0, tiled=True),
    )
    mlp_set = (
        lax.all_gather(gain_mlp, "dp", axis=0, tiled=True),
        lax.all_gather(w_gate, "dp", axis=0, tiled=True),
        lax.all_gather(w_up, "dp", axis=0, tiled=True),
        lax.all_gather(w_down, "dp", axis=0, tiled=True),
    )
    gain_one, wqkv_full, bqkv_full, wout_full = attn_set
    gain_two, wgate_full, wup_full, wdown_full = mlp_set
    hidden_in = inputs.astype(jnp.float32)
    positions = lax.axis_index("seq") * tokens + jnp.arange(tokens, dtype=jnp.int32)
    cosine_tab, sine_tab = rope_tables(positions)
    cos_b = cosine_tab[:, None, :]
    sin_b = sine_tab[:, None, :]
    normed, norm_pull = jax.vjp(rms_scale, hidden_in, gain_one.astype(jnp.float32))
    normed_low = normed.astype(jnp.bfloat16)
    projected = jnp.dot(
        normed_low, wqkv_full, preferred_element_type=jnp.float32
    ) + bqkv_full.astype(jnp.float32)
    queries = projected[:, :q_width].reshape(tokens, HEADS, HEAD_DIM)
    keys_pre = projected[:, q_width : q_width + kv_width].reshape(tokens, KV_HEADS, HEAD_DIM)
    values_pre = projected[:, q_width + kv_width :].reshape(tokens, KV_HEADS, HEAD_DIM)
    queries_low = rotate(queries, cos_b, sin_b).astype(jnp.bfloat16)
    keys_low = jnp.repeat(rotate(keys_pre, cos_b, sin_b), repeat, axis=1).astype(jnp.bfloat16)
    values_low = jnp.repeat(values_pre, repeat, axis=1).astype(jnp.bfloat16)
    query_heads, key_heads, value_heads = (
        lax.all_to_all(queries_low, "seq", split_axis=1, concat_axis=0, tiled=True),
        lax.all_to_all(keys_low, "seq", split_axis=1, concat_axis=0, tiled=True),
        lax.all_to_all(values_low, "seq", split_axis=1, concat_axis=0, tiled=True),
    )
    attended, log_totals = attend_forward(query_heads, key_heads, value_heads)
    attended_tok = lax.all_to_all(attended, "seq", split_axis=0, concat_axis=1, tiled=True)
    attended_flat = attended_tok.reshape(tokens, q_width)
    middle = hidden_in + jnp.dot(attended_flat, wout_full, preferred_element_type=jnp.float32)
    normed_two, norm_two_pull = jax.vjp(rms_scale, middle, gain_two.astype(jnp.float32))
    normed_two_low = normed_two.astype(jnp.bfloat16)
    gate_pre = jnp.dot(normed_two_low, wgate_full, preferred_element_type=jnp.float32)
    up_proj = jnp.dot(normed_two_low, wup_full, preferred_element_type=jnp.float32)
    activated, act_pull = jax.vjp(
        lambda gate_in, up_in: jax.nn.silu(gate_in) * up_in, gate_pre, up_proj
    )
    activated_low = activated.astype(jnp.bfloat16)
    mlp_out = jnp.dot(activated_low, wdown_full, preferred_element_type=jnp.float32)
    output = (middle + mlp_out).astype(jnp.bfloat16)
    attn_back = (
        lax.all_gather(gain_attn, "dp", axis=0, tiled=True),
        lax.all_gather(w_qkv, "dp", axis=0, tiled=True),
        lax.all_gather(b_qkv, "dp", axis=0, tiled=True),
        lax.all_gather(w_out, "dp", axis=0, tiled=True),
    )
    mlp_back = (
        lax.all_gather(gain_mlp, "dp", axis=0, tiled=True),
        lax.all_gather(w_gate, "dp", axis=0, tiled=True),
        lax.all_gather(w_up, "dp", axis=0, tiled=True),
        lax.all_gather(w_down, "dp", axis=0, tiled=True),
    )
    wqkv_back = attn_back[1]
    wout_back = attn_back[3]
    wgate_back = mlp_back[1]
    wup_back = mlp_back[2]
    wdown_back = mlp_back[3]
    grad_out = cotangent.astype(jnp.float32)
    grad_act = times_trans(cotangent, wdown_back)
    grad_gate, grad_up = act_pull(grad_act)
    grad_gate_low = grad_gate.astype(jnp.bfloat16)
    grad_up_low = grad_up.astype(jnp.bfloat16)
    grad_normed_two = times_trans(grad_gate_low, wgate_back) + times_trans(grad_up_low, wup_back)
    grad_middle_norm, grad_gain_two = norm_two_pull(grad_normed_two)
    grad_middle = grad_out + grad_middle_norm
    grad_middle_low = grad_middle.astype(jnp.bfloat16)
    grad_attended = times_trans(grad_middle_low, wout_back).astype(jnp.bfloat16)
    grad_heads_in = lax.all_to_all(
        grad_attended.reshape(tokens, HEADS, HEAD_DIM),
        "seq",
        split_axis=1,
        concat_axis=0,
        tiled=True,
    )
    grad_q, grad_k, grad_v = attend_backward(
        query_heads, key_heads, value_heads, log_totals, grad_heads_in
    )
    grad_q_tok, grad_k_tok, grad_v_tok = (
        lax.all_to_all(grad_q, "seq", split_axis=0, concat_axis=1, tiled=True),
        lax.all_to_all(grad_k, "seq", split_axis=0, concat_axis=1, tiled=True),
        lax.all_to_all(grad_v, "seq", split_axis=0, concat_axis=1, tiled=True),
    )
    grad_k_sum = jnp.sum(
        grad_k_tok.astype(jnp.float32).reshape(tokens, KV_HEADS, repeat, HEAD_DIM), axis=2
    )
    grad_v_sum = jnp.sum(
        grad_v_tok.astype(jnp.float32).reshape(tokens, KV_HEADS, repeat, HEAD_DIM), axis=2
    )
    grad_q_pre = unrotate(grad_q_tok.astype(jnp.float32), cos_b, sin_b)
    grad_k_pre = unrotate(grad_k_sum, cos_b, sin_b)
    grad_proj = jnp.concatenate(
        [
            grad_q_pre.reshape(tokens, q_width),
            grad_k_pre.reshape(tokens, kv_width),
            grad_v_sum.reshape(tokens, kv_width),
        ],
        axis=1,
    ).astype(jnp.bfloat16)
    grad_normed = times_trans(grad_proj, wqkv_back)
    grad_hidden_norm, grad_gain_one = norm_pull(grad_normed)
    grad_inputs = grad_middle + grad_hidden_norm
    term_wqkv = trans_times(normed_low, grad_proj)
    term_bqkv = jnp.sum(grad_proj.astype(jnp.float32), axis=0)
    term_wout = trans_times(attended_flat, grad_middle_low)
    sum_gain_one, sum_wqkv, sum_bqkv, sum_wout, sum_gain_two = (
        lax.psum_scatter(
            grad_gain_one.astype(jnp.bfloat16), "dp", scatter_dimension=0, tiled=True
        ).astype(jnp.float32),
        lax.psum_scatter(
            term_wqkv.astype(jnp.bfloat16), "dp", scatter_dimension=0, tiled=True
        ).astype(jnp.float32),
        lax.psum_scatter(
            term_bqkv.astype(jnp.bfloat16), "dp", scatter_dimension=0, tiled=True
        ).astype(jnp.float32),
        lax.psum_scatter(
            term_wout.astype(jnp.bfloat16), "dp", scatter_dimension=0, tiled=True
        ).astype(jnp.float32),
        lax.psum_scatter(
            grad_gain_two.astype(jnp.bfloat16), "dp", scatter_dimension=0, tiled=True
        ).astype(jnp.float32),
    )
    gate_up_low = jnp.concatenate([grad_gate_low, grad_up_low], axis=1)
    columns = normed_two_low
    sum_gate_up = lax.psum_scatter(
        trans_times(columns, gate_up_low).astype(jnp.bfloat16),
        "dp",
        scatter_dimension=0,
        tiled=True,
    )
    columns = activated_low
    sum_down = lax.psum_scatter(
        trans_times(columns, cotangent).astype(jnp.bfloat16), "dp", scatter_dimension=0, tiled=True
    )
    totals = (
        lax.psum(sum_gain_one.astype(jnp.bfloat16), "seq").astype(jnp.float32),
        lax.psum(sum_wqkv.astype(jnp.bfloat16), "seq").astype(jnp.float32),
        lax.psum(sum_bqkv.astype(jnp.bfloat16), "seq").astype(jnp.float32),
        lax.psum(sum_wout.astype(jnp.bfloat16), "seq").astype(jnp.float32),
        lax.psum(sum_gain_two.astype(jnp.bfloat16), "seq").astype(jnp.float32),
        lax.psum(sum_gate_up, "seq").astype(jnp.float32),
        lax.psum(sum_down, "seq").astype(jnp.float32),
    )
    grad_gate_up = totals[5]
    return (
        output,
        grad_inputs,
        totals[0],
        totals[1],
        totals[2],
        totals[3],
        totals[4],
        grad_gate_up[:, :ff_width],
        grad_gate_up[:, ff_width:],
        totals[6],
    )


Z_LEN = 4
X_LEN = 2
SEQ_PARTS = 4
MESH = pl.DeviceIdType.MESH
HBM = pl.BlockSpec(memory_space=pl.ANY)
VMEM = pl.BlockSpec(memory_space=pltpu.VMEM)
BF16 = jnp.bfloat16
F32 = jnp.float32


def place():
    dp = lax.axis_index("dp")
    part = lax.axis_index("seq")
    z, x = lax.div(dp, X_LEN), lax.rem(dp, X_LEN)
    return dp, part, z, x


def quarter_of(part):
    y, core = lax.div(part, 2), lax.rem(part, 2)
    return (1 - y) * 3 * core + y * (1 + core)


def turn(value, step, length):
    return lax.rem(value + step, length)


def remote(source, target, send, recv, dp, part):
    return pltpu.make_async_remote_copy(
        src_ref=source,
        dst_ref=target,
        send_sem=send,
        recv_sem=recv,
        device_id=(dp, part),
        device_id_type=MESH,
    )


def block(index, size):
    return pl.ds(pl.multiple_of(index * size, size), size)


def greet(partners):
    barrier = pltpu.get_barrier_semaphore()
    for dp, part in partners:
        pl.semaphore_signal(barrier, inc=1, device_id=(dp, part), device_id_type=MESH)
    pl.semaphore_wait(barrier, len(partners))


def z_partners(dp, part, z, x):
    return [(turn(z, step, Z_LEN) * X_LEN + x, part) for step in range(1, Z_LEN)]


def seq_partners(dp, part):
    return [(dp, turn(part, step, SEQ_PARTS)) for step in range(1, SEQ_PARTS)]


class RowGather:
    def __init__(self, source, dest, send, recv, local, base):
        self.source, self.dest, self.send, self.recv, self.local, self.base = (
            source, dest, send, recv, local, base,
        )
        self.rows = dest.shape[0] // X_LEN

    def slot(self, x):
        return self.dest.at[block(x, self.rows)]

    def copy(self, source, slot, send, recv, dp, part):
        return remote(
            source, slot, self.send.at[self.base + send], self.recv.at[self.base + recv], dp, part
        )

    def start(self):
        dp, part, z, x = place()
        quarter = quarter_of(part)
        mine = self.slot(x)

        @pl.when(z == quarter)
        def _():
            pltpu.make_async_copy(self.source, mine, self.local).start()
            for step in range(1, Z_LEN):
                self.copy(
                    self.source, mine, step - 1, 0, turn(z, step, Z_LEN) * X_LEN + x, part
                ).start()
            self.copy(self.source, mine, 3, 1, z * X_LEN + 1 - x, part).start()

    def relay(self):
        dp, part, z, x = place()
        mine = self.slot(x)

        @pl.when(z != quarter_of(part))
        def _():
            self.copy(mine, mine, 0, 0, dp, part).wait_recv()
            self.copy(mine, mine, 3, 1, z * X_LEN + 1 - x, part).start()

    def arrive(self):
        dp, part, z, x = place()
        mine, other = self.slot(x), self.slot(1 - x)

        @pl.when(z == quarter_of(part))
        def _():
            pltpu.make_async_copy(self.source, mine, self.local).wait()

        self.copy(other, other, 3, 1, dp, part).wait_recv()

    def drain(self):
        dp, part, z, x = place()
        mine = self.slot(x)

        @pl.when(z == quarter_of(part))
        def _():
            for step in range(1, Z_LEN):
                self.copy(self.source, mine, step - 1, 0, dp, part).wait_send()

        self.copy(self.source, mine, 3, 1, dp, part).wait_send()


def over_rows(count, step, work):
    def one(index, carry):
        work(pl.ds(pl.multiple_of(index * step, step), step))
        return carry

    lax.fori_loop(0, count // step, one, 0)


def mean_square(value):
    return lax.rsqrt(jnp.mean(value * value, axis=-1, keepdims=True) + NORM_EPS)


def rms_back(value, grad, gain):
    scale = mean_square(value)
    unit = value * scale
    pulled = grad * gain
    inner = jnp.mean(pulled * unit, axis=-1, keepdims=True)
    return scale * (pulled - unit * inner), grad * unit


NT = (((1,), (1,)), ((), ()))
NN = (((1,), (0,)), ((), ()))


def dot(left, right, dims=NN):
    return lax.dot_general(left, right, dims, preferred_element_type=F32)


def loop(count, work):
    def one(index, carry):
        work(index)
        return carry

    lax.fori_loop(0, count, one, 0)


def lanes(rows):
    return lax.broadcasted_iota(jnp.int32, (rows, 128), 1)


def turned(value):
    low_half = lax.rem(lanes(value.shape[0]), HEAD_DIM) < HEAD_DIM // 2
    return jnp.where(low_half, -pltpu.roll(value, 96, axis=1), pltpu.roll(value, 32, axis=1))


def turned_back(value):
    low_half = lax.rem(lanes(value.shape[0]), HEAD_DIM) < HEAD_DIM // 2
    return jnp.where(low_half, pltpu.roll(value, 96, axis=1), -pltpu.roll(value, 32, axis=1))


def sigmoid(value):
    return 1.0 / (1.0 + jnp.exp(-value))


def transpose_into(target, source):
    def work(index):
        target[block(index, 128), :] = source[:, block(index, 128)].T

    loop(source.shape[1] // 128, work)


class ColumnGather:
    def __init__(self, dest, send, recv, base):
        self.dest, self.send, self.recv, self.base = dest, send, recv, base
        self.rows = dest.shape[0] // (Z_LEN * X_LEN)

    def slot(self, dp):
        return self.dest.at[block(dp, self.rows)]

    def copy(self, slot, index, dp, part):
        return remote(
            slot, slot, self.send.at[self.base + index], self.recv.at[self.base + index], dp, part
        )

    def start_z(self):
        dp, part, z, x = place()
        for step in range(1, Z_LEN):
            self.copy(self.slot(dp), step - 1, turn(z, step, Z_LEN) * X_LEN + x, part).start()

    def start_x(self):
        dp, part, z, x = place()
        self.copy(self.slot(dp), 3, z * X_LEN + 1 - x, part).start()

    def relay(self, steps=range(1, Z_LEN)):
        dp, part, z, x = place()
        for step in steps:
            slot = self.slot(turn(z, Z_LEN - step, Z_LEN) * X_LEN + x)
            self.copy(slot, step - 1, dp, part).wait_recv()
            self.copy(slot, 3 + step, z * X_LEN + 1 - x, part).start()

    def arrive(self):
        dp, part, z, x = place()
        for step in range(Z_LEN):
            slot = self.slot(turn(z, Z_LEN - step, Z_LEN) * X_LEN + 1 - x)
            self.copy(slot, 3 + step, dp, part).wait_recv()

    def drain(self):
        dp, part, z, x = place()
        for index in range(7):
            self.copy(self.slot(dp), index, dp, part).wait_send()


class SeqGather:
    def __init__(self, dest, send, recv, base):
        self.dest, self.send, self.recv, self.base = dest, send, recv, base
        self.rows = dest.shape[0] // SEQ_PARTS

    def copy(self, slot, index, dp, part):
        where = self.dest.at[block(slot, self.rows)]
        return remote(
            where, where, self.send.at[self.base + index], self.recv.at[self.base + index], dp, part
        )

    def start(self):
        dp, part, z, x = place()
        for step in range(1, SEQ_PARTS):
            self.copy(part, step - 1, dp, turn(part, step, SEQ_PARTS)).start()

    def arrive(self):
        dp, part, z, x = place()
        for step in range(1, SEQ_PARTS):
            self.copy(turn(part, SEQ_PARTS - step, SEQ_PARTS), step - 1, dp, part).wait_recv()

    def drain(self):
        dp, part, z, x = place()
        for step in range(1, SEQ_PARTS):
            self.copy(part, step - 1, dp, part).wait_send()


class SeqReduce:
    def __init__(self, own, outbox, inbox, send, recv, base):
        self.own, self.outbox, self.inbox = own, outbox, inbox
        self.send, self.recv, self.base = send, recv, base

    def copy(self, index, dp, part):
        return remote(
            self.outbox.at[index],
            self.inbox.at[index],
            self.send.at[self.base + index],
            self.recv.at[self.base + index],
            dp,
            part,
        )

    def start(self, left, right, dims):
        dp, part, z, x = place()
        rows = self.own.shape[0]
        for first in (1, 3):
            near, far = [turn(part, first + each, SEQ_PARTS) for each in range(2)]
            both = jnp.concatenate([left[block(near, rows), :], left[block(far, rows), :]], axis=0)
            value = dot(both, right[...], dims)
            self.outbox[first - 1] = value[:rows].astype(BF16)
            self.copy(first - 1, dp, near).start()
            if first == 1:
                self.outbox[first] = value[rows:].astype(BF16)
                self.copy(first, dp, far).start()
            else:
                self.own[...] = value[rows:]

    def arrive(self):
        dp, part, z, x = place()
        for step in range(SEQ_PARTS - 1):
            self.copy(step, dp, part).wait_recv()

    def total(self, rows):
        value = self.own[rows, :]
        for step in range(SEQ_PARTS - 1):
            value = value + self.inbox[step, rows, :].astype(F32)
        return value

    def drain(self):
        dp, part, z, x = place()
        for step in range(SEQ_PARTS - 1):
            self.copy(step, dp, part).wait_send()


class ColumnReduce:
    def __init__(self, outbox, keep, xbox, hold, zbox, send, recv, base):
        self.outbox, self.keep, self.xbox, self.hold, self.zbox = outbox, keep, xbox, hold, zbox
        self.send, self.recv, self.base = send, recv, base
        self.rows = keep.shape[1]

    def copy(self, source, slot, index, dp, part):
        return remote(
            source, slot, self.send.at[self.base + index], self.recv.at[self.base + index], dp, part
        )

    def cross(self, step):
        dp, part, z, x = place()
        return self.copy(
            self.outbox.at[step], self.xbox.at[step], step, z * X_LEN + 1 - x, part
        )

    def along(self, step):
        dp, part, z, x = place()
        return self.copy(
            self.hold.at[step - 1],
            self.zbox.at[step - 1],
            3 + step,
            turn(z, step, Z_LEN) * X_LEN + x,
            part,
        )

    def start(self, left, right):
        dp, part, z, x = place()
        for step in range(Z_LEN - 1, -1, -1):
            target = turn(z, step, Z_LEN) * X_LEN
            both = jnp.concatenate(
                [left[block(target + 1 - x, self.rows), :], left[block(target + x, self.rows), :]],
                axis=0,
            )
            value = dot(both, right[...])
            self.outbox[step] = value[: self.rows].astype(BF16)
            self.cross(step).start()
            self.keep[step] = value[self.rows :]

    def relay(self, step):
        self.cross(step).wait_recv()

        def work(rows):
            value = self.keep[step, rows, :] + self.xbox[step, rows, :].astype(F32)
            if step:
                self.hold[step - 1, rows, :] = value.astype(BF16)
            else:
                self.keep[step, rows, :] = value

        over_rows(self.rows, 16, work)
        if step:
            self.along(step).start()

    def arrive(self):
        for step in range(1, Z_LEN):
            self.along(step).wait_recv()

    def total(self, rows):
        value = self.keep[0, rows, :]
        for step in range(Z_LEN - 1):
            value = value + self.zbox[step, rows, :].astype(F32)
        return value.astype(BF16)

    def drain(self):
        for step in range(Z_LEN):
            self.cross(step).wait_send()
        for step in range(1, Z_LEN):
            self.along(step).wait_send()


class RowReduce:
    def __init__(self, grads, outbox, xbox, hold, zbox, out, send, recv, base):
        self.grads, self.outbox, self.xbox = grads, outbox, xbox
        self.hold, self.zbox, self.out = hold, zbox, out
        self.send, self.recv, self.base = send, recv, base
        self.rows = out.shape[0]

    def copy(self, source, slot, send, recv, dp, part):
        return remote(
            source, slot, self.send.at[self.base + send], self.recv.at[self.base + recv], dp, part
        )

    def cross(self):
        dp, part, z, x = place()
        return self.copy(self.outbox, self.xbox, 0, 0, z * X_LEN + 1 - x, part)

    def along(self, step):
        dp, part, z, x = place()
        return self.copy(
            self.hold, self.zbox.at[step - 1], 1, 1 + step, quarter_of(part) * X_LEN + x, part
        )

    def share(self, step, source_part):
        dp, part, z, x = place()
        return self.copy(self.out, self.out, 1 + step, 5, dp, turn(source_part, step, SEQ_PARTS))

    def here(self, x, rows):
        return pl.ds(pl.multiple_of(x * self.rows + rows.start, 16), 16)

    def start(self):
        dp, part, z, x = place()

        def work(rows):
            self.outbox[rows, :] = self.grads[self.here(1 - x, rows), :].astype(BF16)

        over_rows(self.rows, 16, work)
        self.cross().start()

    def relay(self):
        dp, part, z, x = place()
        self.cross().wait_recv()
        gap = turn(quarter_of(part), Z_LEN - z, Z_LEN)

        def value(rows):
            return self.grads[self.here(x, rows), :] + self.xbox[rows, :].astype(F32)

        @pl.when(gap == 0)
        def _():
            def work(rows):
                self.grads[self.here(x, rows), :] = value(rows)

            over_rows(self.rows, 16, work)

        @pl.when(gap != 0)
        def _():
            def work(rows):
                self.hold[rows, :] = value(rows).astype(BF16)

            over_rows(self.rows, 16, work)

        for step in range(1, Z_LEN):

            @pl.when(gap == step)
            def _(step=step):
                self.along(step).start()

    def finish(self):
        dp, part, z, x = place()

        @pl.when(z == quarter_of(part))
        def _():
            for step in range(1, Z_LEN):
                self.along(step).wait_recv()

            def work(rows):
                value = self.grads[self.here(x, rows), :]
                for step in range(Z_LEN - 1):
                    value = value + self.zbox[step, rows, :].astype(F32)
                self.out[rows, :] = value.astype(BF16)

            over_rows(self.rows, 16, work)
            for step in range(1, SEQ_PARTS):
                self.share(step, part).start()

    def drain(self):
        dp, part, z, x = place()
        self.cross().wait_send()

        @pl.when(z == quarter_of(part))
        def _():
            for step in range(1, SEQ_PARTS):
                self.share(step, part).wait_send()

        @pl.when(z != quarter_of(part))
        def _():
            self.along(1).wait_send()
            self.copy(self.out, self.out, 1, 5, dp, part).wait_recv()


class VectorReduce:
    def __init__(self, vector, seq_box, dp_box, out, send, recv, base):
        self.vector, self.seq_box, self.dp_box, self.out = vector, seq_box, dp_box, out
        self.send, self.recv, self.base = send, recv, base
        self.rows = vector.shape[0] // (Z_LEN * X_LEN)

    def copy(self, source, slot, index, dp, part):
        return remote(
            source, slot, self.send.at[self.base + index], self.recv.at[self.base + index], dp, part
        )

    def near(self, step):
        dp, part, z, x = place()
        return self.copy(
            self.seq_box.at[part], self.seq_box.at[part], step, dp, turn(part, step, SEQ_PARTS)
        )

    def far(self, step):
        dp, part, z, x = place()
        target = turn(dp, step, Z_LEN * X_LEN)
        return self.copy(
            self.vector.at[block(target, self.rows)], self.dp_box.at[dp], 4 + step, target, part
        )

    def start(self):
        dp, part, z, x = place()
        self.seq_box[part] = self.vector[...]
        for step in range(1, SEQ_PARTS):
            self.near(step).start()

    def relay(self):
        dp, part, z, x = place()
        for step in range(1, SEQ_PARTS):
            slot = self.seq_box.at[turn(part, SEQ_PARTS - step, SEQ_PARTS)]
            self.copy(slot, slot, step, dp, part).wait_recv()
        value = self.seq_box[0]
        for step in range(1, SEQ_PARTS):
            value = value + self.seq_box[step]
        self.vector[...] = value
        self.dp_box[dp] = self.vector[block(dp, self.rows), :]
        for step in range(1, Z_LEN * X_LEN):
            self.far(step).start()

    def finish(self):
        dp, part, z, x = place()
        count = Z_LEN * X_LEN
        for step in range(1, count):
            slot = self.dp_box.at[turn(dp, count - step, count)]
            self.copy(slot, slot, 4 + step, dp, part).wait_recv()
        value = self.dp_box[0]
        for step in range(1, count):
            value = value + self.dp_box[step]
        self.out[...] = value

    def drain(self):
        for step in range(1, SEQ_PARTS):
            self.near(step).wait_send()
        for step in range(1, Z_LEN * X_LEN):
            self.far(step).wait_send()


class Share:
    def __init__(self, piece_of, send, recv, base):
        self.piece_of, self.send, self.recv, self.base = piece_of, send, recv, base

    def copy(self, index, owner, dp, part):
        piece = self.piece_of(owner)
        return remote(
            piece, piece, self.send.at[self.base + index], self.recv.at[self.base + index], dp, part
        )

    def start(self):
        dp, part, z, x = place()
        for step in range(1, SEQ_PARTS):
            self.copy(step - 1, part, dp, turn(part, step, SEQ_PARTS)).start()

    def finish(self):
        dp, part, z, x = place()
        for step in range(1, SEQ_PARTS):
            self.copy(step - 1, turn(part, SEQ_PARTS - step, SEQ_PARTS), dp, part).wait_recv()
        for step in range(1, SEQ_PARTS):
            self.copy(step - 1, part, dp, part).wait_send()


def layer_kernel(
    x_in, cot, small, w_qkv, w_out, w_gate, w_up, w_down, cos_ref, sin_ref,
    out, grad_in, vec_out, o_qkv, o_out, o_gate, o_up, o_down,
    x_all, cot_all, small_all, small_f, gains, bias_rows, edge, wqkv, wout, wgu, wdown,
    n1, n1t, n2, n2t, gb, q_b, k_b, v_b, qt, att, att_t, norm_log, mid,
    gu_f, act, act_t, ggu, down_f, wout_f, g_att, gat, gpr, gkt, gvt, gmid,
    own_mid, own_gn2, own_out, own_gn1, outbox, inbox,
    down_o, down_x, down_h, down_z, gu_o, gu_k, gu_x, gu_h, gu_z,
    wout_o, wout_x, wout_h, wout_z, qkv_o, qkv_k, qkv_x, qkv_h, qkv_z,
    tail_box, gain_sum, vector, seq_box, dp_box, send, recv, local,
):
    dp, part, z, x = place()
    quarter = quarter_of(part)
    odd = lax.rem(quarter, 2)
    rows = x_in.shape[0]
    width = x_in.shape[1]
    tokens = rows * SEQ_PARTS
    inner = wout.shape[0]
    ff_part = w_gate.shape[1] // SEQ_PARTS
    whole = ff_part // 128 * 128
    padded = act.shape[1]
    half = 64
    own_rows = block(part, rows)

    greet(
        [(turn(dp, step, Z_LEN * X_LEN), part) for step in range(1, Z_LEN * X_LEN)]
        + seq_partners(dp, part)
    )

    loads = []

    def load(source, target):
        copy = pltpu.make_async_copy(source, target, local.at[len(loads)])
        copy.start()
        loads.append(copy)
        return copy

    def gate_start(q):
        return pl.multiple_of(q * ff_part + half * lax.rem(q, 2), 128)

    def edge_start(q):
        return pl.multiple_of(lax.div(q, 2) * 2 * ff_part + whole, 128)

    load(x_in, x_all.at[own_rows])
    load(small, small_all.at[block(dp, small.shape[0])])
    for kind in range(3):
        load(
            w_qkv.at[:, pl.ds(pl.multiple_of(kind * width + quarter * inner, 128), inner)],
            wqkv.at[block(dp, w_qkv.shape[0]), pl.ds(kind * inner, inner)],
        )
    load(cot, cot_all.at[own_rows])
    for kind, source in enumerate((w_gate, w_up)):
        load(
            source.at[:, pl.ds(gate_start(quarter), whole)],
            wgu.at[block(dp, source.shape[0]), pl.ds(kind * whole, whole)],
        )
    for kind, source in enumerate((w_gate, w_up)):
        load(source.at[:, pl.ds(edge_start(quarter), 128)], edge.at[kind])

    x_move = SeqGather(x_all, send, recv, 0)
    cot_move = SeqGather(cot_all, send, recv, 3)
    small_move = ColumnGather(small_all, send, recv, 8)
    qkv_move = ColumnGather(wqkv, send, recv, 16)
    wout_move = RowGather(w_out, wout, send, recv, local.at[14], 24)
    gu_move = ColumnGather(wgu, send, recv, 32)
    wdown_move = RowGather(w_down, wdown.at[pl.ds(0, ff_part)], send, recv, local.at[15], 40)

    loads[0].wait()
    x_move.start()
    loads[1].wait()
    small_move.start_z()
    small_move.start_x()
    for each in loads[2:5]:
        each.wait()
    qkv_move.start_z()
    qkv_move.start_x()
    wout_move.start()
    for each in loads[5:]:
        each.wait()
    cot_move.start()
    low_lanes = lanes(w_gate.shape[0]) < half
    gate_edge, up_edge = edge[0].astype(F32), edge[1].astype(F32)
    even_edge = jnp.where(low_lanes, gate_edge, pltpu.roll(up_edge, half, axis=1))
    odd_edge = jnp.where(low_lanes, pltpu.roll(gate_edge, half, axis=1), up_edge)
    wgu[block(dp, w_gate.shape[0]), pl.ds(2 * whole, 128)] = jnp.where(
        odd == 0, even_edge, odd_edge
    ).astype(BF16)
    small_move.relay()
    gu_move.start_z()
    wdown_move.start()
    small_move.arrive()

    small_f[...] = small_all[...].astype(F32)
    step16 = small.shape[0]
    for shard in range(Z_LEN * X_LEN):
        for kind in range(2):
            gains[pl.ds(kind, 1), pl.ds(shard * 128, 128)] = small_f[
                pl.ds(shard * step16 + kind, 1), :
            ]
        for kind in range(3):
            bias_rows[pl.ds(shard * 3 + kind, 1), :] = small_f[
                pl.ds(shard * step16 + 2 + kind, 1), :
            ]
    gain_one, gain_two = gains[pl.ds(0, 1), :], gains[pl.ds(1, 1), :]

    x_move.arrive()

    def norm_one(rows_now):
        value = x_all[rows_now, :].astype(F32)
        n1[rows_now, :] = (value * mean_square(value) * gain_one).astype(BF16)

    over_rows(tokens, 32, norm_one)
    transpose_into(n1t, n1)
    qkv_move.relay()
    gu_move.start_x()
    qkv_move.arrive()

    def project(rows_now):
        for kind, target in enumerate((q_b, k_b, v_b)):
            value = dot(n1[rows_now, :], wqkv[:, pl.ds(kind * inner, inner)])
            for piece in range(inner // 128):
                row = kind * (width // 128) + quarter * (inner // 128) + piece
                bit = value[:, piece * 128 : piece * 128 + 128] + bias_rows[pl.ds(row, 1), :]
                if kind < 2:
                    bit = bit * cos_ref[rows_now, :] + turned(bit) * sin_ref[rows_now, :]
                target[rows_now, pl.ds(piece * 128, 128)] = bit.astype(BF16)

    over_rows(tokens, 256, project)
    wout_move.relay()

    scale = 1.0 / math.sqrt(HEAD_DIM)
    span = tokens // 2

    def head_parts(head):
        tile = block(lax.div(head, 2), 128)
        mask = lax.div(lanes(span), HEAD_DIM) == lax.rem(head, 2)
        return tile, mask

    def scores(query_rows, keys, first):
        value = dot(query_rows, keys, NT) * scale
        row = lax.broadcasted_iota(jnp.int32, value.shape, 0) + first
        column = lax.broadcasted_iota(jnp.int32, value.shape, 1)
        return jnp.where(row >= column, value, MASK_LOW)

    def forward_head(head):
        tile, mask = head_parts(head)
        for first in (0, span):
            near = pl.ds(first, span)
            seen = pl.ds(0, first + span)
            query_rows = jnp.where(mask, q_b[near, tile], jnp.zeros((), BF16))
            value = scores(query_rows, k_b[seen, tile], first)
            top = jnp.max(value, axis=-1, keepdims=True)
            lifted = jnp.exp(value - top)
            total = jnp.sum(lifted, axis=-1, keepdims=True)
            chances = (lifted / total).astype(BF16)
            result = dot(chances, v_b[seen, tile]).astype(BF16)
            att[near, tile] = jnp.where(mask, result, att[near, tile])
            norm_log[head, near, :] = jnp.broadcast_to(top + jnp.log(total), (span, 128))

    att[...] = jnp.zeros_like(att)
    loop(HEADS // SEQ_PARTS, forward_head)
    wout_move.arrive()

    mid_move = SeqReduce(own_mid, outbox.at[0], inbox.at[0], send, recv, 48)
    mid_move.start(att, wout, NN)
    transpose_into(att_t, att)
    transpose_into(qt, q_b)
    cot_move.arrive()
    mid_move.arrive()
    n2_move = SeqGather(n2, send, recv, 51)

    def norm_two(rows_now):
        here = pl.ds(pl.multiple_of(part * rows + rows_now.start, 16), 16)
        value = x_all[here, :].astype(F32) + mid_move.total(rows_now)
        mid[rows_now, :] = value
        n2[here, :] = (value * mean_square(value) * gain_two).astype(BF16)

    over_rows(rows, 16, norm_two)
    n2_move.start()
    n2_move.arrive()
    transpose_into(n2t, n2)
    gu_move.relay()
    gu_move.arrive()

    def feed(rows_now):
        value = dot(n2[rows_now, :], wgu[...])
        gu_f[rows_now, :] = value
        gate, up = value[:, :whole], value[:, whole : 2 * whole]
        act[rows_now, pl.ds(0, whole)] = (gate * sigmoid(gate) * up).astype(BF16)
        last = value[:, 2 * whole :]
        low = lanes(last.shape[0]) < half
        product = last * sigmoid(last) * pltpu.roll(last, half, axis=1)
        act[rows_now, pl.ds(whole, 128)] = jnp.where(low, product, 0.0).astype(BF16)

    over_rows(tokens, 256, feed)
    transpose_into(act_t, act)
    down_move = RowReduce(down_f, down_o, down_x, down_h, down_z, o_down, send, recv, 60)

    front = pl.multiple_of(half * odd, half)

    def down_term(index):
        value = dot(act_t[block(index, 256), :], cot_all[...])
        down_f[pl.ds(pl.multiple_of(front + index * 256, half), 256), :] = value

    loop(whole // 256, down_term)
    value = dot(act_t[pl.ds(whole // 256 * 256, 256), :], cot_all[...])
    down_f[pl.ds(pl.multiple_of(front + whole // 256 * 256, half), 128), :] = value[:128]
    down_f[pl.ds(pl.multiple_of((1 - odd) * whole, half), half), :] = value[128 : 128 + half]
    down_move.start()

    wdown_move.relay()
    wdown_move.arrive()
    wdown[pl.ds(ff_part, half), :] = wdown[pl.ds(0, half), :]
    wdown[pl.ds(ff_part + half, half), :] = jnp.zeros((half, width), BF16)
    down_view = wdown.at[pl.ds(front, padded)]

    def feed_back(rows_now):
        grad = dot(cot_all[rows_now, :], down_view[...], NT)
        value = gu_f[rows_now, :]
        gate, up = value[:, :whole], value[:, whole : 2 * whole]
        some = sigmoid(gate)
        grad_whole = grad[:, :whole]
        ggu[rows_now, pl.ds(0, whole)] = (
            grad_whole * up * (some * (1.0 + gate * (1.0 - some)))
        ).astype(BF16)
        ggu[rows_now, pl.ds(whole, whole)] = (grad_whole * (gate * some)).astype(BF16)
        last = value[:, 2 * whole :]
        swapped = pltpu.roll(last, half, axis=1)
        grad_last = grad[:, whole:]
        low = lanes(last.shape[0]) < half
        some = sigmoid(last)
        ggu[rows_now, pl.ds(2 * whole, 128)] = jnp.where(
            low,
            grad_last * swapped * (some * (1.0 + last * (1.0 - some))),
            pltpu.roll(grad_last, half, axis=1) * (swapped * sigmoid(swapped)),
        ).astype(BF16)

    over_rows(tokens, 128, feed_back)
    gn2_move = SeqReduce(own_gn2, outbox.at[1], inbox.at[1], send, recv, 66)
    gn2_move.start(ggu, wgu, NT)
    gu_grad = ColumnReduce(gu_o, gu_k, gu_x, gu_h, gu_z, send, recv, 72)
    gu_grad.start(n2t, ggu)
    down_move.relay()
    out_move = SeqReduce(own_out, outbox.at[2], inbox.at[2], send, recv, 80)
    out_move.start(act, down_view, NN)

    gn2_move.arrive()
    gb_move = SeqGather(gb, send, recv, 84)
    gain_sum[...] = jnp.zeros_like(gain_sum)

    def mid_back(rows_now):
        here = pl.ds(pl.multiple_of(part * rows + rows_now.start, 16), 16)
        pulled, summand = rms_back(mid[rows_now, :], gn2_move.total(rows_now), gain_two)
        total = cot_all[here, :].astype(F32) + pulled
        gmid[rows_now, :] = total
        gb[here, :] = total.astype(BF16)
        gain_sum[pl.ds(8, 8), :] += jnp.sum(summand.reshape(2, 8, width), axis=0)

    over_rows(rows, 16, mid_back)
    gb_move.start()
    gu_grad.relay(3)
    out_move.arrive()

    def emit(rows_now):
        out[rows_now, :] = (mid[rows_now, :] + out_move.total(rows_now)).astype(BF16)

    over_rows(rows, 16, emit)
    gb_move.arrive()

    def att_back(rows_now):
        g_att[rows_now, :] = dot(gb[rows_now, :], wout[...], NT).astype(BF16)

    over_rows(tokens, 256, att_back)
    transpose_into(gat, g_att)
    gu_grad.relay(2)

    def backward_head(head):
        tile, mask = head_parts(head)
        mine = block(head, HEAD_DIM)
        for first in (0, span):
            near = pl.ds(first, span)
            seen = pl.ds(0, first + span)
            query_rows = jnp.where(mask, q_b[near, tile], jnp.zeros((), BF16))
            value = scores(query_rows, k_b[seen, tile], first)
            log_total = norm_log[head, near, :][:, :1]
            chances = jnp.exp(value - log_total)
            part_v = dot(gat[mine, near], chances.astype(BF16))
            grad_rows = jnp.where(mask, g_att[near, tile], jnp.zeros((), BF16))
            grad_chances = dot(grad_rows, v_b[seen, tile], NT)
            inner_sum = jnp.sum(chances * grad_chances, axis=-1, keepdims=True)
            grad_scores = (chances * (grad_chances - inner_sum)).astype(BF16)
            part_q = dot(grad_scores, k_b[seen, tile]) * scale
            part_q = part_q.astype(BF16).astype(F32)
            old = gpr[near, tile].astype(F32)
            gpr[near, tile] = jnp.where(mask, part_q, old).astype(BF16)
            part_k = dot(qt[mine, near], grad_scores) * scale
            if first == 0:
                gkt[mine, pl.ds(0, span)] = part_k
                gvt[mine, pl.ds(0, span)] = part_v
            else:
                gkt[mine, pl.ds(0, span)] += part_k[:, :span]
                gvt[mine, pl.ds(0, span)] += part_v[:, :span]
                gkt[mine, pl.ds(span, span)] = part_k[:, span:]
                gvt[mine, pl.ds(span, span)] = part_v[:, span:]

    gpr[:, pl.ds(0, inner)] = jnp.zeros((tokens, inner), BF16)
    per_half = HEADS // SEQ_PARTS // 2
    loop(per_half, backward_head)
    gu_grad.relay(1)
    loop(per_half, lambda head: backward_head(head + per_half))

    def settle(index):
        tile = block(index, 128)
        for kind, source in ((1, gkt), (2, gvt)):
            value = source[tile, :].astype(BF16).T
            gpr[:, pl.ds(pl.multiple_of(kind * inner + index * 128, 128), 128)] = value

    loop(inner // 128, settle)

    def unturn(index):
        tile = block(index, 128)
        value = gpr[:, tile].astype(F32)
        gpr[:, tile] = (
            value * cos_ref[...] + turned_back(value * sin_ref[...])
        ).astype(BF16)

    loop(2 * inner // 128, unturn)
    wout_f[...] = dot(att_t[...], gb[...])
    wout_grad = RowReduce(wout_f, wout_o, wout_x, wout_h, wout_z, o_out, send, recv, 88)
    qkv_grad = ColumnReduce(qkv_o, qkv_k, qkv_x, qkv_h, qkv_z, send, recv, 96)
    wout_grad.start()
    qkv_grad.start(n1t, gpr)
    gn1_move = SeqReduce(own_gn1, outbox.at[3], inbox.at[3], send, recv, 104)
    gn1_move.start(gpr, wqkv, NT)
    gu_grad.relay(0)
    down_move.finish()
    wout_grad.relay()

    gu_grad.arrive()

    def gu_sum(rows_now):
        value = gu_grad.total(rows_now)
        o_gate[rows_now, pl.ds(gate_start(quarter), whole)] = value[:, :whole]
        o_up[rows_now, pl.ds(gate_start(quarter), whole)] = value[:, whole : 2 * whole]
        tail_box[part, rows_now, :] = value[:, 2 * whole :]

    over_rows(gu_grad.rows, 16, gu_sum)
    shares = [
        Share(lambda p: o_gate.at[:, pl.ds(gate_start(quarter_of(p)), whole)], send, recv, 108),
        Share(lambda p: o_up.at[:, pl.ds(gate_start(quarter_of(p)), whole)], send, recv, 111),
        Share(lambda p: tail_box.at[p], send, recv, 114),
    ]
    for share in shares:
        share.start()
    for step in range(Z_LEN - 1, -1, -1):
        qkv_grad.relay(step)

    gn1_move.arrive()

    def first_back(rows_now):
        here = pl.ds(pl.multiple_of(part * rows + rows_now.start, 16), 16)
        pulled, summand = rms_back(
            x_all[here, :].astype(F32), gn1_move.total(rows_now), gain_one
        )
        grad_in[rows_now, :] = gmid[rows_now, :] + pulled
        gain_sum[pl.ds(0, 8), :] += jnp.sum(summand.reshape(2, 8, width), axis=0)

    over_rows(rows, 16, first_back)

    vector[...] = jnp.zeros_like(vector)
    first_gain = jnp.sum(gain_sum[pl.ds(0, 8), :], axis=0, keepdims=True)
    second_gain = jnp.sum(gain_sum[pl.ds(8, 8), :], axis=0, keepdims=True)
    for shard in range(Z_LEN * X_LEN):
        vector[pl.ds(shard * 8, 1), :] = first_gain[:, shard * 128 : shard * 128 + 128]
        vector[pl.ds(shard * 8 + 1, 1), :] = second_gain[:, shard * 128 : shard * 128 + 128]
    for kind in range(3):
        for piece in range(inner // 128):
            column = kind * inner + piece * 128
            row = kind * (width // 128) + quarter * (inner // 128) + piece
            vector[pl.ds(lax.div(row, 3) * 8 + 2 + lax.rem(row, 3), 1), :] = jnp.sum(
                gpr[:, column : column + 128].astype(F32), axis=0, keepdims=True
            )
    vector_move = VectorReduce(vector, seq_box, dp_box, vec_out, send, recv, 117)
    vector_move.start()
    vector_move.relay()
    wout_grad.finish()
    qkv_grad.arrive()

    def qkv_spot(p, kind):
        return pl.ds(pl.multiple_of(kind * width + quarter_of(p) * inner, 128), inner)

    def qkv_sum(rows_now):
        value = qkv_grad.total(rows_now)
        for kind in range(3):
            o_qkv[rows_now, qkv_spot(part, kind)] = value[:, kind * inner : (kind + 1) * inner]

    over_rows(qkv_grad.rows, 16, qkv_sum)
    for kind in range(3):
        share = Share(lambda p, kind=kind: o_qkv.at[:, qkv_spot(p, kind)], send, recv, 130 + 3 * kind)
        share.start()
        shares.append(share)
    vector_move.finish()
    for share in shares:
        share.finish()
    low = lanes(rows) < half
    order = [0, 2, 3, 1]
    for pair in range(2):
        even = tail_box[order[2 * pair]].astype(F32)
        uneven = tail_box[order[2 * pair + 1]].astype(F32)
        spot = pl.ds(pair * 2 * ff_part + whole, 128)
        o_gate[:, spot] = jnp.where(low, even, pltpu.roll(uneven, half, axis=1)).astype(BF16)
        o_up[:, spot] = jnp.where(low, pltpu.roll(even, half, axis=1), uneven).astype(BF16)
    for move in (
        x_move, cot_move, small_move, qkv_move, wout_move, gu_move, wdown_move,
        mid_move, n2_move, gn2_move, out_move, gb_move, gn1_move,
        down_move, gu_grad, wout_grad, qkv_grad, vector_move,
    ):
        move.drain()


def ring_body(inputs, gain_attn, w_qkv, b_qkv, w_out, gain_mlp, w_gate, w_up, w_down, cotangent):
    rows, width = inputs.shape
    count = Z_LEN * X_LEN
    inner = HEADS // SEQ_PARTS * HEAD_DIM
    ff_part = w_gate.shape[1] // SEQ_PARTS
    padded = (ff_part + 127) // 128 * 128
    tokens = rows * SEQ_PARTS
    small = jnp.concatenate(
        [
            gain_attn.reshape(1, 128),
            gain_mlp.reshape(1, 128),
            b_qkv.reshape(3, 128),
            jnp.zeros((11, 128), BF16),
        ]
    )
    cosine_tab, sine_tab = rope_tables(jnp.arange(tokens, dtype=jnp.int32))
    cos_two = jnp.concatenate([cosine_tab, cosine_tab], axis=1)
    sin_two = jnp.concatenate([sine_tab, sine_tab], axis=1)

    def vm(*shape, dtype=BF16):
        return pltpu.VMEM(shape, dtype)

    gu_wide, qkv_wide = 2 * ff_part, 3 * inner
    down_rows, out_rows, shard = w_down.shape[0], w_out.shape[0], w_qkv.shape[0]
    scratch = [
        vm(tokens, width), vm(tokens, width), vm(count * 16, 128), vm(count * 16, 128, dtype=F32),
        vm(8, width, dtype=F32), vm(24, 128, dtype=F32), vm(2, shard, 128),
        vm(width, qkv_wide), vm(inner, width), vm(width, gu_wide), vm(padded + 64, width),
        vm(tokens, width), vm(width, tokens), vm(tokens, width), vm(width, tokens),
        vm(tokens, width), vm(tokens, inner), vm(tokens, inner), vm(tokens, inner),
        vm(inner, tokens), vm(tokens, inner), vm(inner, tokens),
        vm(HEADS // SEQ_PARTS, tokens, 128, dtype=F32), vm(rows, width, dtype=F32),
        vm(tokens, gu_wide, dtype=F32), vm(tokens, padded), vm(padded, tokens),
        vm(tokens, gu_wide), vm(ff_part, width, dtype=F32), vm(inner, width, dtype=F32),
        vm(tokens, inner), vm(inner, tokens), vm(tokens, qkv_wide),
        vm(inner, tokens, dtype=F32), vm(inner, tokens, dtype=F32), vm(rows, width, dtype=F32),
    ]
    scratch += [vm(rows, width, dtype=F32)] * 4
    scratch += [vm(4, SEQ_PARTS - 1, rows, width)] * 2
    scratch += [vm(down_rows, width)] * 3 + [vm(Z_LEN - 1, down_rows, width)]
    scratch += [
        vm(Z_LEN, shard, gu_wide), vm(Z_LEN, shard, gu_wide, dtype=F32), vm(Z_LEN, shard, gu_wide),
        vm(Z_LEN - 1, shard, gu_wide), vm(Z_LEN - 1, shard, gu_wide),
    ]
    scratch += [vm(out_rows, width)] * 3 + [vm(Z_LEN - 1, out_rows, width)]
    scratch += [
        vm(Z_LEN, shard, qkv_wide), vm(Z_LEN, shard, qkv_wide, dtype=F32), vm(Z_LEN, shard, qkv_wide),
        vm(Z_LEN - 1, shard, qkv_wide), vm(Z_LEN - 1, shard, qkv_wide),
    ]
    scratch += [
        vm(SEQ_PARTS, shard, 128), vm(16, width, dtype=F32), vm(count * 8, 128, dtype=F32),
        vm(SEQ_PARTS, count * 8, 128, dtype=F32), vm(count, 8, 128, dtype=F32),
        pltpu.SemaphoreType.DMA((140,)), pltpu.SemaphoreType.DMA((140,)),
        pltpu.SemaphoreType.DMA((16,)),
    ]
    output, grad_inputs, sums, g_qkv, g_out, g_gate, g_up, g_down = pl.pallas_call(
        layer_kernel,
        out_shape=(
            jax.ShapeDtypeStruct((rows, width), BF16),
            jax.ShapeDtypeStruct((rows, width), F32),
            jax.ShapeDtypeStruct((8, 128), F32),
            jax.ShapeDtypeStruct(w_qkv.shape, BF16),
            jax.ShapeDtypeStruct(w_out.shape, BF16),
            jax.ShapeDtypeStruct(w_gate.shape, BF16),
            jax.ShapeDtypeStruct(w_up.shape, BF16),
            jax.ShapeDtypeStruct(w_down.shape, BF16),
        ),
        in_specs=[HBM] * 8 + [VMEM] * 2,
        out_specs=[VMEM] * 8,
        scratch_shapes=scratch,
        compiler_params=pltpu.CompilerParams(
            collective_id=0, has_side_effects=True, vmem_limit_bytes=67043328
        ),
    )(inputs, cotangent, small, w_qkv, w_out, w_gate, w_up, w_down, cos_two, sin_two)
    return (
        output,
        grad_inputs,
        sums[0],
        g_qkv.astype(F32),
        sums[2:5].reshape(-1),
        g_out.astype(F32),
        sums[1],
        g_gate.astype(F32),
        g_up.astype(F32),
        g_down.astype(F32),
    )


def solution(mesh):
    tuned = mesh.shape["dp"] == Z_LEN * X_LEN and mesh.shape["seq"] == SEQ_PARTS
    return jax.shard_map(
        ring_body if tuned else generic_body,
        mesh=mesh,
        in_specs=(
            P(("dp", "seq"), None),
            P("dp"),
            P("dp", None),
            P("dp"),
            P("dp", None),
            P("dp"),
            P("dp", None),
            P("dp", None),
            P("dp", None),
            P(("dp", "seq"), None),
        ),
        out_specs=(
            P(("dp", "seq"), None),
            P(("dp", "seq"), None),
            P("dp"),
            P("dp", None),
            P("dp"),
            P("dp", None),
            P("dp"),
            P("dp", None),
            P("dp", None),
            P("dp", None),
        ),
        check_vma=False,
    )
```

```python
import math

import jax
import numpy as np
import jax.numpy as jnp
from jax import lax
from jax.experimental import pallas as pl
from jax.experimental.pallas import tpu as pltpu
from jax.sharding import PartitionSpec as P

HEADS = 16
KV_HEADS = 16
HEAD_DIM = 64


NORM_EPS = 1e-06
ROPE_BASE = 1000000.0
MASK_LOW = -1000000000.0


def rms_scale(signal, gain_vec):
    return (
        signal * lax.rsqrt(jnp.mean(signal * signal, axis=-1, keepdims=True) + NORM_EPS) * gain_vec
    )


def rotate(signal, cosine_tab, sine_tab):
    half_dim = signal.shape[-1] // 2
    turned = jnp.concatenate([-signal[..., half_dim:], signal[..., :half_dim]], axis=-1)
    return signal * cosine_tab + turned * sine_tab


def unrotate(grad_in, cosine_tab, sine_tab):
    half_dim = grad_in.shape[-1] // 2
    shifted = grad_in * sine_tab
    flipped = jnp.concatenate([shifted[..., half_dim:], -shifted[..., :half_dim]], axis=-1)
    return grad_in * cosine_tab + flipped


def rope_tables(positions):
    inverse_freq = 1.0 / ROPE_BASE ** (jnp.arange(0, HEAD_DIM, 2).astype(jnp.float32) / HEAD_DIM)
    angles = positions.astype(jnp.float32)[:, None] * inverse_freq[None, :]
    cosine_tab = jnp.cos(angles)
    sine_tab = jnp.sin(angles)
    return (
        jnp.concatenate([cosine_tab, cosine_tab], axis=-1),
        jnp.concatenate([sine_tab, sine_tab], axis=-1),
    )


def times_trans(left_op, weight):
    return lax.dot_general(
        left_op, weight, (((1,), (1,)), ((), ())), preferred_element_type=jnp.float32
    )


def trans_times(left_op, right_op):
    return lax.dot_general(
        left_op, right_op, (((0,), (0,)), ((), ())), preferred_element_type=jnp.float32
    )


def masked_scores(query_rows, keys_all, block_index, block_len):
    length = keys_all.shape[0]
    score_scale = 1.0 / math.sqrt(HEAD_DIM)
    scores = (
        jnp.einsum("qhe,khe->hqk", query_rows, keys_all, preferred_element_type=jnp.float32)
        * score_scale
    )
    query_pos = block_index * block_len + jnp.arange(block_len)
    key_pos = jnp.arange(length)
    return jnp.where(query_pos[:, None] >= key_pos[None, :], scores, MASK_LOW)


def attend_forward(queries, keys_all, values_all):
    length = queries.shape[0]
    block_len = min(512, length)
    block_count = length // block_len

    def one_block(block_index):
        scores = masked_scores(queries, keys_all, block_index, block_len)
        row_top = jnp.max(scores, axis=-1, keepdims=True)
        lifted = jnp.exp(scores - row_top)
        row_total = jnp.sum(lifted, axis=-1, keepdims=True)
        chances = (lifted / row_total).astype(jnp.bfloat16)
        block_out = jnp.einsum(
            "hqk,khe->qhe", chances, values_all, preferred_element_type=jnp.float32
        ).astype(jnp.bfloat16)
        log_total = (row_top + jnp.log(row_total))[..., 0]
        return (block_out, log_total)

    outs_all, log_totals = lax.map(one_block, jnp.arange(block_count))
    return (outs_all.reshape(queries.shape), log_totals)


def attend_backward(queries, keys_all, values_all, log_totals, grad_rows_all):
    length = queries.shape[0]
    block_len = min(512, length)
    block_count = length // block_len
    score_scale = 1.0 / math.sqrt(HEAD_DIM)

    def one_block(running, block_index):
        grad_keys, grad_values = running
        scores = masked_scores(queries, keys_all, block_index, block_len)
        log_total = lax.dynamic_index_in_dim(log_totals, block_index, 0, keepdims=False)
        chances = jnp.exp(scores - log_total[..., None])
        chances_low = chances.astype(jnp.bfloat16)
        grad_values = grad_values + jnp.einsum(
            "hqk,qhe->khe", chances_low, grad_rows_all, preferred_element_type=jnp.float32
        )
        grad_chances = jnp.einsum(
            "qhe,khe->hqk", grad_rows_all, values_all, preferred_element_type=jnp.float32
        )
        inner_sum = jnp.sum(chances * grad_chances, axis=-1, keepdims=True)
        grad_scores = (chances * (grad_chances - inner_sum)).astype(jnp.bfloat16)
        grad_query = (
            jnp.einsum("hqk,khe->qhe", grad_scores, keys_all, preferred_element_type=jnp.float32)
            * score_scale
        ).astype(jnp.bfloat16)
        grad_keys = (
            grad_keys
            + jnp.einsum("hqk,qhe->khe", grad_scores, queries, preferred_element_type=jnp.float32)
            * score_scale
        )
        return ((grad_keys, grad_values), grad_query)

    zeros_kv = jnp.zeros(keys_all.shape, jnp.float32)
    (grad_keys, grad_values), grad_queries = lax.scan(
        one_block, (zeros_kv, zeros_kv), jnp.arange(block_count)
    )
    return (
        grad_queries.reshape(queries.shape),
        grad_keys.astype(jnp.bfloat16),
        grad_values.astype(jnp.bfloat16),
    )


def generic_body(inputs, gain_attn, w_qkv, b_qkv, w_out, gain_mlp, w_gate, w_up, w_down, cotangent):
    tokens = inputs.shape[0]
    repeat = HEADS // KV_HEADS
    q_width = HEADS * HEAD_DIM
    kv_width = KV_HEADS * HEAD_DIM
    ff_width = w_gate.shape[1]
    attn_set = (
        lax.all_gather(gain_attn, "dp", axis=0, tiled=True),
        lax.all_gather(w_qkv, "dp", axis=0, tiled=True),
        lax.all_gather(b_qkv, "dp", axis=0, tiled=True),
        lax.all_gather(w_out, "dp", axis=0, tiled=True),
    )
    mlp_set = (
        lax.all_gather(gain_mlp, "dp", axis=0, tiled=True),
        lax.all_gather(w_gate, "dp", axis=0, tiled=True),
        lax.all_gather(w_up, "dp", axis=0, tiled=True),
        lax.all_gather(w_down, "dp", axis=0, tiled=True),
    )
    gain_one, wqkv_full, bqkv_full, wout_full = attn_set
    gain_two, wgate_full, wup_full, wdown_full = mlp_set
    hidden_in = inputs.astype(jnp.float32)
    positions = lax.axis_index("seq") * tokens + jnp.arange(tokens, dtype=jnp.int32)
    cosine_tab, sine_tab = rope_tables(positions)
    cos_b = cosine_tab[:, None, :]
    sin_b = sine_tab[:, None, :]
    normed, norm_pull = jax.vjp(rms_scale, hidden_in, gain_one.astype(jnp.float32))
    normed_low = normed.astype(jnp.bfloat16)
    projected = jnp.dot(
        normed_low, wqkv_full, preferred_element_type=jnp.float32
    ) + bqkv_full.astype(jnp.float32)
    queries = projected[:, :q_width].reshape(tokens, HEADS, HEAD_DIM)
    keys_pre = projected[:, q_width : q_width + kv_width].reshape(tokens, KV_HEADS, HEAD_DIM)
    values_pre = projected[:, q_width + kv_width :].reshape(tokens, KV_HEADS, HEAD_DIM)
    queries_low = rotate(queries, cos_b, sin_b).astype(jnp.bfloat16)
    keys_low = jnp.repeat(rotate(keys_pre, cos_b, sin_b), repeat, axis=1).astype(jnp.bfloat16)
    values_low = jnp.repeat(values_pre, repeat, axis=1).astype(jnp.bfloat16)
    query_heads, key_heads, value_heads = (
        lax.all_to_all(queries_low, "seq", split_axis=1, concat_axis=0, tiled=True),
        lax.all_to_all(keys_low, "seq", split_axis=1, concat_axis=0, tiled=True),
        lax.all_to_all(values_low, "seq", split_axis=1, concat_axis=0, tiled=True),
    )
    attended, log_totals = attend_forward(query_heads, key_heads, value_heads)
    attended_tok = lax.all_to_all(attended, "seq", split_axis=0, concat_axis=1, tiled=True)
    attended_flat = attended_tok.reshape(tokens, q_width)
    middle = hidden_in + jnp.dot(attended_flat, wout_full, preferred_element_type=jnp.float32)
    normed_two, norm_two_pull = jax.vjp(rms_scale, middle, gain_two.astype(jnp.float32))
    normed_two_low = normed_two.astype(jnp.bfloat16)
    gate_pre = jnp.dot(normed_two_low, wgate_full, preferred_element_type=jnp.float32)
    up_proj = jnp.dot(normed_two_low, wup_full, preferred_element_type=jnp.float32)
    activated, act_pull = jax.vjp(
        lambda gate_in, up_in: jax.nn.silu(gate_in) * up_in, gate_pre, up_proj
    )
    activated_low = activated.astype(jnp.bfloat16)
    mlp_out = jnp.dot(activated_low, wdown_full, preferred_element_type=jnp.float32)
    output = (middle + mlp_out).astype(jnp.bfloat16)
    attn_back = (
        lax.all_gather(gain_attn, "dp", axis=0, tiled=True),
        lax.all_gather(w_qkv, "dp", axis=0, tiled=True),
        lax.all_gather(b_qkv, "dp", axis=0, tiled=True),
        lax.all_gather(w_out, "dp", axis=0, tiled=True),
    )
    mlp_back = (
        lax.all_gather(gain_mlp, "dp", axis=0, tiled=True),
        lax.all_gather(w_gate, "dp", axis=0, tiled=True),
        lax.all_gather(w_up, "dp", axis=0, tiled=True),
        lax.all_gather(w_down, "dp", axis=0, tiled=True),
    )
    wqkv_back = attn_back[1]
    wout_back = attn_back[3]
    wgate_back = mlp_back[1]
    wup_back = mlp_back[2]
    wdown_back = mlp_back[3]
    grad_out = cotangent.astype(jnp.float32)
    grad_act = times_trans(cotangent, wdown_back)
    grad_gate, grad_up = act_pull(grad_act)
    grad_gate_low = grad_gate.astype(jnp.bfloat16)
    grad_up_low = grad_up.astype(jnp.bfloat16)
    grad_normed_two = times_trans(grad_gate_low, wgate_back) + times_trans(grad_up_low, wup_back)
    grad_middle_norm, grad_gain_two = norm_two_pull(grad_normed_two)
    grad_middle = grad_out + grad_middle_norm
    grad_middle_low = grad_middle.astype(jnp.bfloat16)
    grad_attended = times_trans(grad_middle_low, wout_back).astype(jnp.bfloat16)
    grad_heads_in = lax.all_to_all(
        grad_attended.reshape(tokens, HEADS, HEAD_DIM),
        "seq",
        split_axis=1,
        concat_axis=0,
        tiled=True,
    )
    grad_q, grad_k, grad_v = attend_backward(
        query_heads, key_heads, value_heads, log_totals, grad_heads_in
    )
    grad_q_tok, grad_k_tok, grad_v_tok = (
        lax.all_to_all(grad_q, "seq", split_axis=0, concat_axis=1, tiled=True),
        lax.all_to_all(grad_k, "seq", split_axis=0, concat_axis=1, tiled=True),
        lax.all_to_all(grad_v, "seq", split_axis=0, concat_axis=1, tiled=True),
    )
    grad_k_sum = jnp.sum(
        grad_k_tok.astype(jnp.float32).reshape(tokens, KV_HEADS, repeat, HEAD_DIM), axis=2
    )
    grad_v_sum = jnp.sum(
        grad_v_tok.astype(jnp.float32).reshape(tokens, KV_HEADS, repeat, HEAD_DIM), axis=2
    )
    grad_q_pre = unrotate(grad_q_tok.astype(jnp.float32), cos_b, sin_b)
    grad_k_pre = unrotate(grad_k_sum, cos_b, sin_b)
    grad_proj = jnp.concatenate(
        [
            grad_q_pre.reshape(tokens, q_width),
            grad_k_pre.reshape(tokens, kv_width),
            grad_v_sum.reshape(tokens, kv_width),
        ],
        axis=1,
    ).astype(jnp.bfloat16)
    grad_normed = times_trans(grad_proj, wqkv_back)
    grad_hidden_norm, grad_gain_one = norm_pull(grad_normed)
    grad_inputs = grad_middle + grad_hidden_norm
    term_wqkv = trans_times(normed_low, grad_proj)
    term_bqkv = jnp.sum(grad_proj.astype(jnp.float32), axis=0)
    term_wout = trans_times(attended_flat, grad_middle_low)
    sum_gain_one, sum_wqkv, sum_bqkv, sum_wout, sum_gain_two = (
        lax.psum_scatter(
            grad_gain_one.astype(jnp.bfloat16), "dp", scatter_dimension=0, tiled=True
        ).astype(jnp.float32),
        lax.psum_scatter(
            term_wqkv.astype(jnp.bfloat16), "dp", scatter_dimension=0, tiled=True
        ).astype(jnp.float32),
        lax.psum_scatter(
            term_bqkv.astype(jnp.bfloat16), "dp", scatter_dimension=0, tiled=True
        ).astype(jnp.float32),
        lax.psum_scatter(
            term_wout.astype(jnp.bfloat16), "dp", scatter_dimension=0, tiled=True
        ).astype(jnp.float32),
        lax.psum_scatter(
            grad_gain_two.astype(jnp.bfloat16), "dp", scatter_dimension=0, tiled=True
        ).astype(jnp.float32),
    )
    gate_up_low = jnp.concatenate([grad_gate_low, grad_up_low], axis=1)
    columns = normed_two_low
    sum_gate_up = lax.psum_scatter(
        trans_times(columns, gate_up_low).astype(jnp.bfloat16),
        "dp",
        scatter_dimension=0,
        tiled=True,
    )
    columns = activated_low
    sum_down = lax.psum_scatter(
        trans_times(columns, cotangent).astype(jnp.bfloat16), "dp", scatter_dimension=0, tiled=True
    )
    totals = (
        lax.psum(sum_gain_one.astype(jnp.bfloat16), "seq").astype(jnp.float32),
        lax.psum(sum_wqkv.astype(jnp.bfloat16), "seq").astype(jnp.float32),
        lax.psum(sum_bqkv.astype(jnp.bfloat16), "seq").astype(jnp.float32),
        lax.psum(sum_wout.astype(jnp.bfloat16), "seq").astype(jnp.float32),
        lax.psum(sum_gain_two.astype(jnp.bfloat16), "seq").astype(jnp.float32),
        lax.psum(sum_gate_up, "seq").astype(jnp.float32),
        lax.psum(sum_down, "seq").astype(jnp.float32),
    )
    grad_gate_up = totals[5]
    return (
        output,
        grad_inputs,
        totals[0],
        totals[1],
        totals[2],
        totals[3],
        totals[4],
        grad_gate_up[:, :ff_width],
        grad_gate_up[:, ff_width:],
        totals[6],
    )


Z_LEN = 4
X_LEN = 2
SEQ_PARTS = 4
MESH = pl.DeviceIdType.MESH
HBM = pl.BlockSpec(memory_space=pl.ANY)
VMEM = pl.BlockSpec(memory_space=pltpu.VMEM)
BF16 = jnp.bfloat16
F32 = jnp.float32


def place():
    dp = lax.axis_index("dp")
    part = lax.axis_index("seq")
    z, x = lax.div(dp, X_LEN), lax.rem(dp, X_LEN)
    return dp, part, z, x


def quarter_of(part):
    y, core = lax.div(part, 2), lax.rem(part, 2)
    return (1 - y) * 3 * core + y * (1 + core)


def turn(value, step, length):
    return lax.rem(value + step, length)


def remote(source, target, send, recv, dp, part):
    return pltpu.make_async_remote_copy(
        src_ref=source,
        dst_ref=target,
        send_sem=send,
        recv_sem=recv,
        device_id=(dp, part),
        device_id_type=MESH,
    )


def block(index, size):
    return pl.ds(pl.multiple_of(index * size, size), size)


def greet(partners):
    barrier = pltpu.get_barrier_semaphore()
    for dp, part in partners:
        pl.semaphore_signal(barrier, inc=1, device_id=(dp, part), device_id_type=MESH)
    pl.semaphore_wait(barrier, len(partners))


def z_partners(dp, part, z, x):
    return [(turn(z, step, Z_LEN) * X_LEN + x, part) for step in range(1, Z_LEN)]


def seq_partners(dp, part):
    return [(dp, turn(part, step, SEQ_PARTS)) for step in range(1, SEQ_PARTS)]


def over_rows(count, step, work):
    def one(index, carry):
        work(pl.ds(pl.multiple_of(index * step, step), step))
        return carry

    lax.fori_loop(0, count // step, one, 0)


def mean_square(value):
    return lax.rsqrt(jnp.mean(value * value, axis=-1, keepdims=True) + NORM_EPS)


def rms_back(value, grad, gain):
    scale = mean_square(value)
    unit = value * scale
    pulled = grad * gain
    inner = jnp.mean(pulled * unit, axis=-1, keepdims=True)
    return scale * (pulled - unit * inner), grad * unit


SEMAPHORES = 139
NT = (((1,), (1,)), ((), ()))
NN = (((1,), (0,)), ((), ()))


def dot(left, right, dims=NN):
    return lax.dot_general(left, right, dims, preferred_element_type=F32)


def loop(count, work):
    def one(index, carry):
        work(index)
        return carry

    lax.fori_loop(0, count, one, 0)


def lanes(rows):
    return lax.broadcasted_iota(jnp.int32, (rows, 128), 1)


def turned(value):
    low_half = lax.rem(lanes(value.shape[0]), HEAD_DIM) < HEAD_DIM // 2
    return jnp.where(low_half, -pltpu.roll(value, 96, axis=1), pltpu.roll(value, 32, axis=1))


def turned_back(value):
    low_half = lax.rem(lanes(value.shape[0]), HEAD_DIM) < HEAD_DIM // 2
    return jnp.where(low_half, pltpu.roll(value, 96, axis=1), -pltpu.roll(value, 32, axis=1))


def sigmoid(value):
    return 1.0 / (1.0 + jnp.exp(-value))


def transpose_into(target, source):
    def work(index):
        target[block(index, 128), :] = source[:, block(index, 128)].T

    loop(source.shape[1] // 128, work)


class RowGather:
    def __init__(self, source, dest, send, recv, local, base, chunks):
        self.source, self.dest, self.send, self.recv, self.local, self.base = (
            source, dest, send, recv, local, base,
        )
        self.chunks = chunks
        self.rows = dest.shape[0] // X_LEN
        self.step = self.rows // chunks

    def slot(self, x, chunk):
        return self.dest.at[pl.ds(pl.multiple_of(x * self.rows + chunk * self.step, 16), self.step)]

    def mine(self, chunk):
        return self.source.at[pl.ds(chunk * self.step, self.step)]

    def copy(self, source, slot, chunk, send, recv, dp, part):
        base = self.base + chunk * 4
        return remote(source, slot, self.send.at[base + send], self.recv.at[base + recv], dp, part)

    def start_x(self):
        dp, part, z, x = place()

        @pl.when(z == quarter_of(part))
        def _():
            pltpu.make_async_copy(
                self.source, self.dest.at[block(x, self.rows)], self.local
            ).start()
            for chunk in range(self.chunks):
                self.copy(
                    self.mine(chunk), self.slot(x, chunk), chunk, 3, 1, z * X_LEN + 1 - x, part
                ).start()

    def start_z(self):
        dp, part, z, x = place()

        @pl.when(z == quarter_of(part))
        def _():
            for chunk in range(self.chunks):
                for step in range(1, Z_LEN):
                    self.copy(
                        self.mine(chunk), self.slot(x, chunk), chunk, step - 1, 0,
                        turn(z, step, Z_LEN) * X_LEN + x, part,
                    ).start()

    def relay(self, chunk):
        dp, part, z, x = place()
        slot = self.slot(x, chunk)

        @pl.when(z != quarter_of(part))
        def _():
            self.copy(slot, slot, chunk, 0, 0, dp, part).wait_recv()
            self.copy(slot, slot, chunk, 3, 1, z * X_LEN + 1 - x, part).start()

    def arrive(self):
        dp, part, z, x = place()

        @pl.when(z == quarter_of(part))
        def _():
            pltpu.make_async_copy(
                self.source, self.dest.at[block(x, self.rows)], self.local
            ).wait()

        for chunk in range(self.chunks):
            slot = self.slot(1 - x, chunk)
            self.copy(slot, slot, chunk, 3, 1, dp, part).wait_recv()

    def drain(self):
        dp, part, z, x = place()

        @pl.when(z == quarter_of(part))
        def _():
            for chunk in range(self.chunks):
                for step in range(1, Z_LEN):
                    self.copy(
                        self.mine(chunk), self.slot(x, chunk), chunk, step - 1, 0, dp, part
                    ).wait_send()

        for chunk in range(self.chunks):
            self.copy(self.mine(chunk), self.slot(x, chunk), chunk, 3, 1, dp, part).wait_send()


class ChainGather(RowGather):
    def up(self, source, chunk, z, x):
        return self.copy(source, self.slot(x, chunk), chunk, 0, 0, z * X_LEN + x, lax.axis_index("seq"))

    def down(self, source, chunk, z, x):
        return self.copy(source, self.slot(x, chunk), chunk, 1, 0, z * X_LEN + x, lax.axis_index("seq"))

    def start_z(self):
        dp, part, z, x = place()
        for chunk in range(self.chunks):

            @pl.when((z == quarter_of(part)) & (z < Z_LEN - 1))
            def _(chunk=chunk):
                self.up(self.mine(chunk), chunk, z + 1, x).start()

            @pl.when((z == quarter_of(part)) & (z > 0))
            def _(chunk=chunk):
                self.down(self.mine(chunk), chunk, z - 1, x).start()

    def relay(self, chunk, hop):
        dp, part, z, x = place()
        quarter = quarter_of(part)
        slot = self.slot(x, chunk)

        @pl.when((z == quarter + hop) | (z == quarter - hop))
        def _():
            self.up(slot, chunk, z, x).wait_recv()

            @pl.when((z > quarter) & (z < Z_LEN - 1))
            def _():
                self.up(slot, chunk, z + 1, x).start()

            @pl.when((z < quarter) & (z > 0))
            def _():
                self.down(slot, chunk, z - 1, x).start()

            if chunk == 0:
                self.cross(chunk)

    def cross(self, chunk):
        dp, part, z, x = place()
        slot = self.slot(x, chunk)
        self.copy(slot, slot, chunk, 3, 1, z * X_LEN + 1 - x, part).start()

    def start_x(self):
        dp, part, z, x = place()

        @pl.when(z == quarter_of(part))
        def _():
            own = pltpu.make_async_copy(self.source, self.dest.at[block(x, self.rows)], self.local)
            own.start()
            own.wait()
            self.cross(0)

    def arrive(self):
        dp, part, z, x = place()
        for chunk in range(self.chunks):
            slot = self.slot(1 - x, chunk)
            self.copy(slot, slot, chunk, 3, 1, dp, part).wait_recv()

    def drain(self):
        dp, part, z, x = place()
        quarter = quarter_of(part)
        for chunk in range(self.chunks):

            @pl.when((z >= quarter) & (z < Z_LEN - 1))
            def _(chunk=chunk):
                self.up(self.mine(chunk), chunk, z, x).wait_send()

            @pl.when((z <= quarter) & (z > 0))
            def _(chunk=chunk):
                self.down(self.mine(chunk), chunk, z, x).wait_send()

            self.copy(self.mine(chunk), self.slot(x, chunk), chunk, 3, 1, dp, part).wait_send()


class ColumnGather:
    def __init__(self, dest, send, recv, base):
        self.dest, self.send, self.recv, self.base = dest, send, recv, base
        self.rows = dest.shape[0] // (Z_LEN * X_LEN)

    def slot(self, z, x):
        return self.dest.at[block(z * X_LEN + x, self.rows)]

    def copy(self, slot, index, z, x):
        part = lax.axis_index("seq")
        return remote(
            slot, slot, self.send.at[self.base + index], self.recv.at[self.base + index],
            z * X_LEN + x, part,
        )

    def start_z(self):
        dp, part, z, x = place()

        @pl.when(z < Z_LEN - 1)
        def _():
            self.copy(self.slot(z, x), 0, z + 1, x).start()

        @pl.when(z > 0)
        def _():
            self.copy(self.slot(z, x), 3, z - 1, x).start()

    def start_x(self):
        dp, part, z, x = place()
        self.copy(self.slot(z, x), 6, z, 1 - x).start()

    def relay(self, hop):
        dp, part, z, x = place()

        @pl.when(z >= hop)
        def _():
            slot = self.slot(z - hop, x)
            self.copy(slot, hop - 1, z, x).wait_recv()
            if hop < Z_LEN - 1:

                @pl.when(z < Z_LEN - 1)
                def _():
                    self.copy(slot, hop, z + 1, x).start()

            self.copy(slot, 6 + hop, z, 1 - x).start()

        @pl.when(z + hop < Z_LEN)
        def _():
            slot = self.slot(z + hop, x)
            self.copy(slot, 2 + hop, z, x).wait_recv()
            if hop < Z_LEN - 1:

                @pl.when(z > 0)
                def _():
                    self.copy(slot, 3 + hop, z - 1, x).start()

            self.copy(slot, 9 + hop, z, 1 - x).start()

    def arrive(self):
        dp, part, z, x = place()
        slot = self.slot(z, 1 - x)
        self.copy(slot, 6, z, x).wait_recv()
        for hop in range(1, Z_LEN):

            @pl.when(z >= hop)
            def _(hop=hop):
                slot = self.slot(z - hop, 1 - x)
                self.copy(slot, 6 + hop, z, x).wait_recv()

            @pl.when(z + hop < Z_LEN)
            def _(hop=hop):
                slot = self.slot(z + hop, 1 - x)
                self.copy(slot, 9 + hop, z, x).wait_recv()

    def drain(self):
        dp, part, z, x = place()
        mine = self.slot(z, x)

        def sent(index):
            self.copy(mine, index, z, x).wait_send()

        sent(6)
        for hop in range(Z_LEN):

            @pl.when(z >= hop)
            def _(hop=hop):
                if hop:
                    sent(6 + hop)
                if hop < Z_LEN - 1:
                    pl.when(z < Z_LEN - 1)(lambda: sent(hop))

            @pl.when(z + hop < Z_LEN)
            def _(hop=hop):
                if hop:
                    sent(9 + hop)
                if hop < Z_LEN - 1:
                    pl.when(z > 0)(lambda: sent(3 + hop))


class DirectGather:
    def __init__(self, dest, send, recv, base):
        self.dest, self.send, self.recv, self.base = dest, send, recv, base
        self.count = Z_LEN * X_LEN
        self.rows = dest.shape[0] // self.count

    def copy(self, owner, step, dp):
        slot = self.dest.at[block(owner, self.rows)]
        return remote(
            slot, slot, self.send.at[self.base + step], self.recv.at[self.base + step],
            dp, lax.axis_index("seq"),
        )

    def start(self):
        dp, part, z, x = place()
        for step in range(1, self.count):
            self.copy(dp, step, turn(dp, step, self.count)).start()

    def arrive(self):
        dp, part, z, x = place()
        for step in range(1, self.count):
            self.copy(turn(dp, self.count - step, self.count), step, dp).wait_recv()

    def drain(self):
        dp, part, z, x = place()
        for step in range(1, self.count):
            self.copy(dp, step, dp).wait_send()


def sibling(part):
    return part + 1 - 2 * lax.rem(part, 2)


def across(part):
    return turn(part, 2, SEQ_PARTS)


class SeqGather:
    def __init__(self, dest, send, recv, base):
        self.dest, self.send, self.recv, self.base = dest, send, recv, base
        self.rows = dest.shape[0] // SEQ_PARTS

    def copy(self, slot, index, dp, part):
        where = self.dest.at[block(slot, self.rows)]
        return remote(
            where, where, self.send.at[self.base + index], self.recv.at[self.base + index], dp, part
        )

    def start(self):
        dp, part, z, x = place()
        self.copy(part, 1, dp, across(part)).start()
        self.copy(part, 0, dp, sibling(part)).start()

    def relay(self):
        dp, part, z, x = place()
        self.copy(across(part), 1, dp, part).wait_recv()
        self.copy(across(part), 2, dp, sibling(part)).start()

    def arrive(self):
        dp, part, z, x = place()
        self.copy(sibling(part), 0, dp, part).wait_recv()
        self.copy(sibling(across(part)), 2, dp, part).wait_recv()

    def drain(self):
        dp, part, z, x = place()
        for index in range(3):
            self.copy(part, index, dp, part).wait_send()


class SeqReduce:
    def __init__(self, own, far, outbox, inbox, y_out, y_in, send, recv, base):
        self.own, self.far, self.outbox, self.inbox = own, far, outbox, inbox
        self.y_out, self.y_in = y_out, y_in
        self.send, self.recv, self.base = send, recv, base

    def near_copy(self, dp, part):
        return remote(
            self.outbox, self.inbox, self.send.at[self.base], self.recv.at[self.base], dp, part
        )

    def far_copy(self, dp, part):
        return remote(
            self.y_out, self.y_in, self.send.at[self.base + 1], self.recv.at[self.base + 1], dp, part
        )

    def start(self, left, right, dims):
        dp, part, z, x = place()
        rows = self.own.shape[0]
        other = sibling(part)

        def product(first, second):
            both = jnp.concatenate(
                [left[block(first, rows), :], left[block(second, rows), :]], axis=0
            )
            return dot(both, right[...], dims)

        value = product(other, across(other))
        self.outbox[0] = value[:rows]
        self.outbox[1] = value[rows:]
        self.near_copy(dp, other).start()
        value = product(part, across(part))
        self.own[...] = value[:rows]
        self.far[...] = value[rows:]

    def relay(self):
        dp, part, z, x = place()
        self.near_copy(dp, part).wait_recv()

        def work(rows):
            self.y_out[rows, :] = (self.far[rows, :] + self.inbox[1, rows, :]).astype(BF16)

        over_rows(self.own.shape[0], 32, work)
        self.far_copy(dp, across(part)).start()

    def arrive(self):
        dp, part, z, x = place()
        self.far_copy(dp, part).wait_recv()

    def total(self, rows):
        return self.own[rows, :] + self.inbox[0, rows, :] + self.y_in[rows, :].astype(F32)

    def drain(self):
        dp, part, z, x = place()
        self.near_copy(dp, part).wait_send()
        self.far_copy(dp, part).wait_send()


class ColumnReduce:
    def __init__(self, outbox, keep, xbox, hold, inbox, send, recv, base):
        self.outbox, self.keep, self.xbox, self.hold, self.inbox = outbox, keep, xbox, hold, inbox
        self.send, self.recv, self.base = send, recv, base
        self.rows = keep.shape[1]

    def copy(self, source, slot, send, recv, z, x):
        return remote(
            source, slot, self.send.at[self.base + send], self.recv.at[self.base + recv],
            z * X_LEN + x, lax.axis_index("seq"),
        )

    def dest(self, step):
        dp, part, z, x = place()
        low = (z < Z_LEN // 2).astype(jnp.int32)
        return (
            (Z_LEN - 1) * low,
            2 * low + (1 - low),
            (1 - z) * low + (5 - z) * (1 - low),
            z,
        )[step]

    def cross(self, step):
        dp, part, z, x = place()
        return self.copy(self.outbox.at[step], self.xbox.at[step], step, step, z, 1 - x)

    def partial(self, slot):
        dp, part, z, x = place()
        return self.copy(self.inbox.at[slot], self.inbox.at[slot], 9, 4 + slot, z, x)

    def onward(self, step):
        dp, part, z, x = place()
        dest = self.dest(step)
        down = (dest < z).astype(jnp.int32)
        target = z + 1 - 2 * down
        last = down * (target == dest).astype(jnp.int32)
        slot = dest * (1 - last) + Z_LEN * last
        return self.copy(self.hold.at[step], self.inbox.at[slot], 9 + step, 4 + slot, target, x)

    def start(self, left, right):
        dp, part, z, x = place()
        for step in range(Z_LEN):
            target = self.dest(step) * X_LEN
            both = jnp.concatenate(
                [left[block(target + 1 - x, self.rows), :], left[block(target + x, self.rows), :]],
                axis=0,
            )
            value = dot(both, right[...])
            self.outbox[step] = value[: self.rows].astype(BF16)
            self.cross(step).start()
            self.keep[step] = value[self.rows :]

    def value(self, step, rows):
        return self.keep[step, rows, :] + self.xbox[step, rows, :].astype(F32)

    def relay_end(self, step):
        dp, part, z, x = place()

        @pl.when((z == 0) | (z == Z_LEN - 1))
        def _():
            self.cross(step).wait_recv()

            def work(rows):
                self.hold[step, rows, :] = self.value(step, rows).astype(BF16)

            over_rows(self.rows, 16, work)
            self.onward(step).start()

    def relay_mid(self, step):
        dp, part, z, x = place()

        @pl.when((z > 0) & (z < Z_LEN - 1))
        def _():
            slot = self.dest(step)
            self.cross(step).wait_recv()
            self.partial(slot).wait_recv()

            def work(rows):
                self.hold[step, rows, :] = (
                    self.value(step, rows) + self.inbox[slot, rows, :].astype(F32)
                ).astype(BF16)

            over_rows(self.rows, 16, work)
            self.onward(step).start()

    def arrive(self):
        dp, part, z, x = place()
        last = Z_LEN - 1
        self.cross(last).wait_recv()

        def work(rows):
            self.keep[last, rows, :] += self.xbox[last, rows, :].astype(F32)

        over_rows(self.rows, 16, work)
        for there, slot in ((z > 0, z), (z < last, Z_LEN)):

            @pl.when(there)
            def _(slot=slot):
                self.partial(slot).wait_recv()

                def add(rows):
                    self.keep[last, rows, :] += self.inbox[slot, rows, :].astype(F32)

                over_rows(self.rows, 16, add)

    def total(self, rows):
        return self.keep[Z_LEN - 1, rows, :].astype(BF16)

    def drain(self):
        for step in range(Z_LEN):
            self.cross(step).wait_send()
        for step in range(Z_LEN - 1):
            self.onward(step).wait_send()


class ChainReduce:
    def __init__(self, grads, first, outbox, inbox, xout, xin, out, send, recv, local, base):
        self.grads, self.first, self.outbox, self.inbox = grads, first, outbox, inbox
        self.xout, self.xin, self.out, self.local = xout, xin, out, local
        self.send, self.recv, self.base = send, recv, base
        self.rows = xout.shape[0]
        self.stride = grads.shape[0] // X_LEN

    def copy(self, source, slot, send, recv, z, x):
        return remote(
            source, slot, self.send.at[self.base + send], self.recv.at[self.base + recv],
            z * X_LEN + x, lax.axis_index("seq"),
        )

    def upward(self, z, x):
        return self.copy(self.outbox, self.inbox.at[0], 0, 0, z, x)

    def downward(self, z, x):
        return self.copy(self.outbox, self.inbox.at[1], 0, 1, z, x)

    def over(self, work):
        for x in range(X_LEN):

            def one(rows, x=x):
                work(
                    pl.ds(pl.multiple_of(rows.start + x * self.stride + self.first, 16), 16),
                    pl.ds(pl.multiple_of(rows.start + x * self.rows, 16), 16),
                )

            over_rows(self.rows, 16, one)

    def fill(self, side):
        def work(here, box):
            value = self.grads[here, :]
            if side is not None:
                value = value + self.inbox[side, box, :].astype(F32)
            self.outbox[box, :] = value.astype(BF16)

        self.over(work)

    def hand_on(self, hop):
        dp, part, z, x = place()
        quarter = quarter_of(part)

        @pl.when((z < quarter) & (z == hop))
        def _():
            if hop:
                self.upward(z, x).wait_recv()
            self.fill(0 if hop else None)
            self.upward(z + 1, x).start()

        @pl.when((z > quarter) & (z == Z_LEN - 1 - hop))
        def _():
            if hop:
                self.downward(z, x).wait_recv()
            self.fill(1 if hop else None)
            self.downward(z - 1, x).start()

    def here(self, x, rows):
        return pl.ds(pl.multiple_of(x * self.stride + self.first + rows.start, 16), 16)

    def swap(self):
        dp, part, z, x = place()
        return self.copy(self.xout, self.xin, 1, 2, z, 1 - x)

    def owner(self, inner):
        dp, part, z, x = place()
        mine = z == quarter_of(part)
        if inner is None:
            return mine
        return mine & ((part >= SEQ_PARTS // 2) if inner else (part < SEQ_PARTS // 2))

    def total(self, inner=None):
        dp, part, z, x = place()

        @pl.when(self.owner(inner))
        def _():
            for side, there in ((0, z > 0), (1, z < Z_LEN - 1)):

                @pl.when(there)
                def _(side=side):
                    (self.downward if side else self.upward)(z, x).wait_recv()

                    def work(here, box):
                        self.grads[here, :] += self.inbox[side, box, :].astype(F32)

                    self.over(work)

            def cast(rows):
                self.xout[rows, :] = self.grads[self.here(1 - x, rows), :].astype(BF16)

            over_rows(self.rows, 16, cast)
            self.swap().start()

    def share(self, index, part, source=None):
        dp, _, z, x = place()
        source = self.out if source is None else source
        return remote(
            source, self.out, self.send.at[self.base + 2 + index],
            self.recv.at[self.base + 3 + index], dp, part,
        )

    def keep(self):
        return pltpu.make_async_copy(self.stage(), self.out, self.local)

    def stage(self):
        return self.outbox.at[pl.ds(0, self.rows)]

    def finish(self, inner=None):
        dp, part, z, x = place()

        @pl.when(self.owner(inner))
        def _():
            self.swap().wait_recv()

            def work(rows):
                value = self.grads[self.here(x, rows), :] + self.xin[rows, :].astype(F32)
                self.outbox[rows, :] = value.astype(BF16)

            over_rows(self.rows, 16, work)
            self.share(1, across(part), self.stage()).start()
            self.share(0, sibling(part), self.stage()).start()
            self.keep().start()

    def pass_on(self):
        dp, part, z, x = place()

        @pl.when(z == quarter_of(across(part)))
        def _():
            self.share(1, part).wait_recv()
            self.share(2, sibling(part)).start()

    def drain(self):
        dp, part, z, x = place()

        @pl.when(z == quarter_of(part))
        def _():
            self.swap().wait_send()
            self.share(1, part, self.stage()).wait_send()
            self.share(0, part, self.stage()).wait_send()
            self.keep().wait()

        @pl.when(z != quarter_of(part))
        def _():
            self.upward(z, x).wait_send()

        @pl.when(z == quarter_of(across(part)))
        def _():
            self.share(2, part).wait_send()

        @pl.when(z == quarter_of(sibling(part)))
        def _():
            self.share(0, part).wait_recv()

        @pl.when(z == quarter_of(sibling(across(part))))
        def _():
            self.share(2, part).wait_recv()


class RowReduce:
    def __init__(self, grads, first, outbox, xbox, hold, zbox, out, send, recv, local, base):
        self.grads, self.first, self.outbox, self.xbox = grads, first, outbox, xbox
        self.hold, self.zbox, self.out, self.local = hold, zbox, out, local
        self.send, self.recv, self.base = send, recv, base
        self.rows = xbox.shape[0]
        self.stride = grads.shape[0] // X_LEN
        self.chunks = 1
        self.step = self.rows

    def copy(self, source, slot, send, recv, dp, part):
        return remote(
            source, slot, self.send.at[self.base + send], self.recv.at[self.base + recv], dp, part
        )

    def piece(self, chunk):
        return pl.ds(chunk * self.step, self.step)

    def cross(self, chunk):
        dp, part, z, x = place()
        piece = self.piece(chunk)
        return self.copy(
            self.outbox.at[piece], self.xbox.at[piece], chunk, chunk, z * X_LEN + 1 - x, part
        )

    def along(self, chunk, step):
        dp, part, z, x = place()
        piece = self.piece(chunk)
        return self.copy(
            self.hold.at[piece],
            self.zbox.at[step - 1, piece],
            1,
            step,
            quarter_of(part) * X_LEN + x,
            part,
        )

    def share(self, index, part, source=None):
        dp, _, z, x = place()
        source = self.out if source is None else source
        return self.copy(source, self.out, 2 + index, 4 + index, dp, part)

    def keep(self):
        return pltpu.make_async_copy(self.hold, self.out, self.local)

    def here(self, x, rows):
        return pl.ds(pl.multiple_of(x * self.stride + self.first + rows.start, 16), 16)

    def over(self, chunk, work):
        def one(index, carry):
            work(pl.ds(pl.multiple_of(chunk * self.step + index * 16, 16), 16))
            return carry

        lax.fori_loop(0, self.step // 16, one, 0)

    def start(self):
        dp, part, z, x = place()
        for chunk in range(self.chunks):

            def work(rows):
                self.outbox[rows, :] = self.grads[self.here(1 - x, rows), :].astype(BF16)

            self.over(chunk, work)
            self.cross(chunk).start()

    def relay(self, chunk):
        dp, part, z, x = place()
        self.cross(chunk).wait_recv()
        gap = turn(quarter_of(part), Z_LEN - z, Z_LEN)

        def value(rows):
            return self.grads[self.here(x, rows), :] + self.xbox[rows, :].astype(F32)

        @pl.when(gap == 0)
        def _():
            def work(rows):
                self.grads[self.here(x, rows), :] = value(rows)

            self.over(chunk, work)

        @pl.when(gap != 0)
        def _():
            def work(rows):
                self.hold[rows, :] = value(rows).astype(BF16)

            self.over(chunk, work)

        for step in range(1, Z_LEN):

            @pl.when(gap == step)
            def _(step=step):
                self.along(chunk, step).start()

    def finish(self):
        dp, part, z, x = place()

        @pl.when(z == quarter_of(part))
        def _():
            for chunk in range(self.chunks):
                for step in range(1, Z_LEN):
                    self.along(chunk, step).wait_recv()

            def work(rows):
                value = self.grads[self.here(x, rows), :]
                for step in range(Z_LEN - 1):
                    value = value + self.zbox[step, rows, :].astype(F32)
                self.hold[rows, :] = value.astype(BF16)

            over_rows(self.rows, 16, work)
            self.share(1, across(part), self.hold).start()
            self.share(0, sibling(part), self.hold).start()
            self.keep().start()

    def pass_on(self):
        dp, part, z, x = place()

        @pl.when(z == quarter_of(across(part)))
        def _():
            self.share(1, part).wait_recv()
            self.share(2, sibling(part)).start()

    def drain(self):
        dp, part, z, x = place()
        for chunk in range(self.chunks):
            self.cross(chunk).wait_send()

        @pl.when(z == quarter_of(part))
        def _():
            self.share(1, part, self.hold).wait_send()
            self.share(0, part, self.hold).wait_send()
            self.keep().wait()

        @pl.when(z != quarter_of(part))
        def _():
            for chunk in range(self.chunks):
                self.along(chunk, 1).wait_send()

        @pl.when(z == quarter_of(across(part)))
        def _():
            self.share(2, part).wait_send()

        @pl.when(z == quarter_of(sibling(part)))
        def _():
            self.share(0, part).wait_recv()

        @pl.when(z == quarter_of(sibling(across(part))))
        def _():
            self.share(2, part).wait_recv()


class VectorReduce:
    def __init__(self, vector, seq_box, dp_box, out, send, recv, base):
        self.vector, self.seq_box, self.dp_box, self.out = vector, seq_box, dp_box, out
        self.send, self.recv, self.base = send, recv, base
        self.rows = vector.shape[0] // (Z_LEN * X_LEN)

    def copy(self, source, slot, index, dp, part):
        return remote(
            source, slot, self.send.at[self.base + index], self.recv.at[self.base + index], dp, part
        )

    def near(self, step):
        dp, part, z, x = place()
        return self.copy(
            self.seq_box.at[part], self.seq_box.at[part], step, dp, turn(part, step, SEQ_PARTS)
        )

    def far(self, step):
        dp, part, z, x = place()
        target = turn(dp, step, Z_LEN * X_LEN)
        return self.copy(
            self.vector.at[block(target, self.rows)], self.dp_box.at[dp], 4 + step, target, part
        )

    def start(self):
        dp, part, z, x = place()
        self.seq_box[part] = self.vector[...]
        for step in range(1, SEQ_PARTS):
            self.near(step).start()

    def relay(self):
        dp, part, z, x = place()
        for step in range(1, SEQ_PARTS):
            slot = self.seq_box.at[turn(part, SEQ_PARTS - step, SEQ_PARTS)]
            self.copy(slot, slot, step, dp, part).wait_recv()
        value = self.seq_box[0]
        for step in range(1, SEQ_PARTS):
            value = value + self.seq_box[step]
        self.vector[...] = value
        self.dp_box[dp] = self.vector[block(dp, self.rows), :]
        for step in range(1, Z_LEN * X_LEN):
            self.far(step).start()

    def finish(self):
        dp, part, z, x = place()
        count = Z_LEN * X_LEN
        for step in range(1, count):
            slot = self.dp_box.at[turn(dp, count - step, count)]
            self.copy(slot, slot, 4 + step, dp, part).wait_recv()
        value = self.dp_box[0]
        for step in range(1, count):
            value = value + self.dp_box[step]
        self.out[...] = value

    def drain(self):
        for step in range(1, SEQ_PARTS):
            self.near(step).wait_send()
        for step in range(1, Z_LEN * X_LEN):
            self.far(step).wait_send()


class Share:
    def __init__(self, stage, piece_of, send, recv, local, base):
        self.stage, self.piece_of, self.local = stage, piece_of, local
        self.send, self.recv, self.base = send, recv, base

    def copy(self, source, index, owner, dp, part):
        return remote(
            source, self.piece_of(owner), self.send.at[self.base + index],
            self.recv.at[self.base + index], dp, part,
        )

    def keep(self):
        return pltpu.make_async_copy(
            self.stage, self.piece_of(lax.axis_index("seq")), self.local
        )

    def start(self):
        dp, part, z, x = place()
        self.copy(self.stage, 1, part, dp, across(part)).start()
        self.copy(self.stage, 0, part, dp, sibling(part)).start()
        self.keep().start()

    def relay(self):
        dp, part, z, x = place()
        other = self.piece_of(across(part))
        self.copy(other, 1, across(part), dp, part).wait_recv()
        self.copy(other, 2, across(part), dp, sibling(part)).start()

    def finish(self):
        dp, part, z, x = place()
        self.copy(self.stage, 0, sibling(part), dp, part).wait_recv()
        self.copy(self.stage, 2, sibling(across(part)), dp, part).wait_recv()
        for index in range(3):
            self.copy(self.stage, index, part, dp, part).wait_send()
        self.keep().wait()


def layer_kernel(
    x_in, cot, w_qkv, w_out, w_gate, w_up, w_down, cos_in, sin_in, gain_a, gain_m, bias_in,
    out, grad_in, vec_out, o_qkv, o_out, o_gate, o_up, o_down,
    x_all, cot_all, small_f, gains, bias_rows, edge, wqkv, wout, wgu, wdown,
    n1, n1t, n2, n2t, gb, q_b, k_b, v_b, qt, att, att_t, norm_log, mid,
    gu_f, act, act_t, ggu, down_f, wout_f, g_att, gat, gpr, gkt, gvt, gmid,
    cos_ref, sin_ref, own, far, outbox, inbox, y_out, y_in,
    down_co, down_ci, down_cx, down_cy, down_o, down_x, down_h, down_z, gu_o, gu_k, gu_x, gu_h, gu_z,
    wout_o, wout_x, wout_h, wout_z, qkv_o, qkv_k, qkv_x, qkv_h, qkv_z,
    tail_box, gu_stage, qkv_stage, out_stage, in_stage, edges, gain_sum, vector, seq_box, dp_box, send, recv, local,
):
    dp, part, z, x = place()
    quarter = quarter_of(part)
    odd = lax.rem(quarter, 2)
    rows = x_in.shape[0]
    width = x_in.shape[1]
    tokens = rows * SEQ_PARTS
    inner = wout.shape[0]
    ff_part = w_gate.shape[1] // SEQ_PARTS
    whole = ff_part // 128 * 128
    padded = act.shape[1]
    half = 64
    own_rows = block(part, rows)

    used = [0]

    def take(count):
        used[0] += count
        return used[0] - count

    loads = []

    def load(source, target):
        copy = pltpu.make_async_copy(source, target, local.at[len(loads)])
        copy.start()
        loads.append(copy)
        return copy

    def gate_start(q):
        return pl.multiple_of(q * ff_part + half * lax.rem(q, 2), 128)

    def edge_start(q):
        return pl.multiple_of(lax.div(q, 2) * 2 * ff_part + whole, 128)

    load(x_in, x_all.at[own_rows])
    for kind in range(3):
        load(
            w_qkv.at[:, pl.ds(pl.multiple_of(kind * width + quarter * inner, 128), inner)],
            wqkv.at[block(dp, w_qkv.shape[0]), pl.ds(kind * inner, inner)],
        )
    for kind, source in enumerate((w_gate, w_up)):
        load(source.at[:, pl.ds(edge_start(quarter), 128)], edge.at[kind])
    for kind, source in enumerate((w_gate, w_up)):
        load(
            source.at[:, pl.ds(gate_start(quarter), whole)],
            wgu.at[block(dp, source.shape[0]), pl.ds(kind * whole, whole)],
        )
    load(cot, cot_all.at[own_rows])
    load(cos_in, cos_ref)
    load(sin_in, sin_ref)
    small_f[block(dp, 8), :] = jnp.concatenate(
        [
            gain_a[...].astype(F32), gain_m[...].astype(F32), bias_in[...].astype(F32),
            jnp.zeros((3, 128), F32),
        ],
        axis=0,
    )
    for each in loads[4:6]:
        each.wait()
    low_lanes = lanes(w_gate.shape[0]) < half
    gate_edge, up_edge = edge[0].astype(F32), edge[1].astype(F32)
    even_edge = jnp.where(low_lanes, gate_edge, pltpu.roll(up_edge, half, axis=1))
    odd_edge = jnp.where(low_lanes, pltpu.roll(gate_edge, half, axis=1), up_edge)
    wgu[block(dp, w_gate.shape[0]), pl.ds(2 * whole, 128)] = jnp.where(
        odd == 0, even_edge, odd_edge
    ).astype(BF16)
    for each in loads[:4]:
        each.wait()

    greet(
        [(turn(dp, step, Z_LEN * X_LEN), part) for step in range(1, Z_LEN * X_LEN)]
        + seq_partners(dp, part)
    )

    x_move = SeqGather(x_all, send, recv, take(3))
    cot_move = SeqGather(cot_all, send, recv, take(3))
    small_move = DirectGather(small_f, send, recv, take(8))
    qkv_move = ColumnGather(wqkv, send, recv, take(13))
    wout_move = RowGather(w_out, wout, send, recv, local.at[14], take(4), 1)
    gu_move = ColumnGather(wgu, send, recv, take(13))
    wdown_move = ChainGather(w_down, wdown.at[pl.ds(0, ff_part)], send, recv, local.at[15], take(8), 2)

    small_move.start()
    qkv_move.start_z()
    qkv_move.start_x()
    x_move.start()
    wout_move.start_x()
    wout_move.start_z()
    for each in loads[6:]:
        each.wait()
    gu_move.start_x()
    qkv_move.relay(1)
    small_move.arrive()
    x_move.relay()

    step16 = small_f.shape[0] // (Z_LEN * X_LEN)
    for shard in range(Z_LEN * X_LEN):
        for kind in range(2):
            gains[pl.ds(kind, 1), pl.ds(shard * 128, 128)] = small_f[
                pl.ds(shard * step16 + kind, 1), :
            ]
        for kind in range(3):
            bias_rows[pl.ds(shard * 3 + kind, 1), :] = small_f[
                pl.ds(shard * step16 + 2 + kind, 1), :
            ]
    gain_one, gain_two = gains[pl.ds(0, 1), :], gains[pl.ds(1, 1), :]

    x_move.arrive()

    def norm_one(rows_now):
        value = x_all[rows_now, :].astype(F32)
        n1[rows_now, :] = (value * mean_square(value) * gain_one).astype(BF16)

    over_rows(tokens, 32, norm_one)
    qkv_move.relay(2)
    gu_move.start_z()
    wdown_move.start_z()
    cot_move.start()
    transpose_into(n1t, n1)
    qkv_move.relay(3)
    qkv_move.arrive()

    def project(rows_now):
        for kind, target in enumerate((q_b, k_b, v_b)):
            value = dot(n1[rows_now, :], wqkv[:, pl.ds(kind * inner, inner)])
            for piece in range(inner // 128):
                row = kind * (width // 128) + quarter * (inner // 128) + piece
                bit = value[:, piece * 128 : piece * 128 + 128] + bias_rows[pl.ds(row, 1), :]
                if kind < 2:
                    bit = bit * cos_ref[rows_now, :] + turned(bit) * sin_ref[rows_now, :]
                target[rows_now, pl.ds(piece * 128, 128)] = bit.astype(BF16)

    over_rows(tokens, 256, project)
    wout_move.relay(0)
    wdown_move.start_x()
    cot_move.relay()
    gu_move.relay(1)
    scale = 1.0 / math.sqrt(HEAD_DIM)
    span = tokens // 2

    def head_parts(head):
        tile = block(lax.div(head, 2), 128)
        mask = lax.div(lanes(span), HEAD_DIM) == lax.rem(head, 2)
        return tile, mask

    def scores(query_rows, keys, first):
        value = dot(query_rows, keys, NT) * scale
        row = lax.broadcasted_iota(jnp.int32, value.shape, 0) + first
        column = lax.broadcasted_iota(jnp.int32, value.shape, 1)
        return jnp.where(row >= column, value, MASK_LOW)

    def forward_head(head):
        tile, mask = head_parts(head)
        for first in (0, span):
            near = pl.ds(first, span)
            seen = pl.ds(0, first + span)
            query_rows = jnp.where(mask, q_b[near, tile], jnp.zeros((), BF16))
            value = scores(query_rows, k_b[seen, tile], first)
            top = jnp.max(value, axis=-1, keepdims=True)
            lifted = jnp.exp(value - top)
            total = jnp.sum(lifted, axis=-1, keepdims=True)
            chances = (lifted / total).astype(BF16)
            result = dot(chances, v_b[seen, tile]).astype(BF16)
            att[near, tile] = jnp.where(mask, result, att[near, tile])
            norm_log[head, near, :] = jnp.broadcast_to(top + jnp.log(total), (span, 128))

    att[...] = jnp.zeros_like(att)
    loop(HEADS // SEQ_PARTS, forward_head)
    wdown_move.relay(0, 1)
    wout_move.arrive()

    def seq_reduce(index, base):
        return SeqReduce(
            own.at[index], far.at[index], outbox.at[index], inbox.at[index],
            y_out.at[index], y_in.at[index], send, recv, base,
        )

    mid_move = seq_reduce(0, take(2))
    mid_move.start(att, wout, NN)
    transpose_into(att_t, att)
    wdown_move.relay(1, 1)
    mid_move.relay()
    gu_move.relay(2)
    transpose_into(qt, q_b)
    cot_move.arrive()
    mid_move.arrive()
    n2_move = SeqGather(n2, send, recv, take(3))

    def norm_two(rows_now):
        here = pl.ds(pl.multiple_of(part * rows + rows_now.start, 16), 16)
        value = x_all[here, :].astype(F32) + mid_move.total(rows_now)
        mid[rows_now, :] = value
        n2[here, :] = (value * mean_square(value) * gain_two).astype(BF16)

    over_rows(rows, 16, norm_two)
    n2_move.start()
    wdown_move.relay(0, 2)
    wdown_move.relay(1, 2)
    gu_move.relay(3)
    wdown_move.relay(0, 3)
    wdown_move.relay(1, 3)
    n2_move.relay()
    wdown_move.cross(1)
    n2_move.arrive()
    transpose_into(n2t, n2)
    gu_move.arrive()

    def feed(rows_now):
        value = dot(n2[rows_now, :], wgu[...])
        gu_f[rows_now, :] = value
        gate, up = value[:, :whole], value[:, whole : 2 * whole]
        act[rows_now, pl.ds(0, whole)] = (gate * sigmoid(gate) * up).astype(BF16)
        last = value[:, 2 * whole :]
        low = lanes(last.shape[0]) < half
        product = last * sigmoid(last) * pltpu.roll(last, half, axis=1)
        act[rows_now, pl.ds(whole, 128)] = jnp.where(low, product, 0.0).astype(BF16)

    over_rows(tokens, 256, feed)
    transpose_into(act_t, act)
    share_rows = w_down.shape[0] // 2
    down_chain = ChainReduce(
        down_f, 0, down_co, down_ci, down_cx, down_cy, o_down.at[pl.ds(0, share_rows)],
        send, recv, local.at[16], take(6),
    )
    down_move = RowReduce(
        down_f, share_rows, down_o, down_x, down_h, down_z,
        o_down.at[pl.ds(share_rows, share_rows)], send, recv, local.at[29], take(7),
    )

    front = pl.multiple_of(half * odd, half)

    def down_term(index):
        value = dot(act_t[block(index, 256), :], cot_all[...])
        down_f[pl.ds(pl.multiple_of(front + index * 256, half), 256), :] = value

    loop(whole // 256, down_term)
    value = dot(act_t[pl.ds(whole // 256 * 256, 256), :], cot_all[...])
    down_f[pl.ds(pl.multiple_of(front + whole // 256 * 256, half), 128), :] = value[:128]
    down_f[pl.ds(pl.multiple_of((1 - odd) * whole, half), half), :] = value[128 : 128 + half]
    down_chain.hand_on(0)
    down_move.start()

    wdown_move.arrive()
    wdown[pl.ds(ff_part, half), :] = wdown[pl.ds(0, half), :]
    wdown[pl.ds(ff_part + half, half), :] = jnp.zeros((half, width), BF16)
    down_view = wdown.at[pl.ds(front, padded)]

    def feed_back(rows_now):
        grad = dot(cot_all[rows_now, :], down_view[...], NT)
        value = gu_f[rows_now, :]
        gate, up = value[:, :whole], value[:, whole : 2 * whole]
        some = sigmoid(gate)
        grad_whole = grad[:, :whole]
        ggu[rows_now, pl.ds(0, whole)] = (
            grad_whole * up * (some * (1.0 + gate * (1.0 - some)))
        ).astype(BF16)
        ggu[rows_now, pl.ds(whole, whole)] = (grad_whole * (gate * some)).astype(BF16)
        last = value[:, 2 * whole :]
        swapped = pltpu.roll(last, half, axis=1)
        grad_last = grad[:, whole:]
        low = lanes(last.shape[0]) < half
        some = sigmoid(last)
        ggu[rows_now, pl.ds(2 * whole, 128)] = jnp.where(
            low,
            grad_last * swapped * (some * (1.0 + last * (1.0 - some))),
            pltpu.roll(grad_last, half, axis=1) * (swapped * sigmoid(swapped)),
        ).astype(BF16)

    over_rows(tokens, 128, feed_back)
    gn2_move = seq_reduce(1, take(2))
    gn2_move.start(ggu, wgu, NT)
    gu_grad = ColumnReduce(gu_o, gu_k, gu_x, gu_h, gu_z, send, recv, take(12))
    gu_grad.start(n2t, ggu)
    gn2_move.relay()
    down_move.relay(0)
    out_move = seq_reduce(2, take(2))
    out_move.start(act, down_view, NN)
    gn2_move.arrive()
    gb_move = SeqGather(gb, send, recv, take(3))
    gain_sum[...] = jnp.zeros_like(gain_sum)

    def mid_back(rows_now):
        here = pl.ds(pl.multiple_of(part * rows + rows_now.start, 16), 16)
        pulled, summand = rms_back(mid[rows_now, :], gn2_move.total(rows_now), gain_two)
        total = cot_all[here, :].astype(F32) + pulled
        gmid[rows_now, :] = total
        gb[here, :] = total.astype(BF16)
        gain_sum[pl.ds(8, 8), :] += jnp.sum(summand.reshape(2, 8, width), axis=0)

    over_rows(rows, 16, mid_back)
    gb_move.start()
    out_move.relay()
    down_chain.hand_on(1)
    gu_grad.relay_end(0)
    gb_move.relay()
    gb_move.arrive()

    wout_f[...] = dot(att_t[...], gb[...])
    wout_grad = ChainReduce(
        wout_f, 0, wout_o, wout_z, wout_h, wout_x, o_out, send, recv, local.at[17], take(6)
    )
    wout_grad.hand_on(0)
    def att_back(rows_now):
        g_att[rows_now, :] = dot(gb[rows_now, :], wout[...], NT).astype(BF16)

    over_rows(tokens, 256, att_back)
    transpose_into(gat, g_att)

    down_chain.hand_on(2)
    def backward_head(head):
        tile, mask = head_parts(head)
        mine = block(head, HEAD_DIM)
        for first in (0, span):
            near = pl.ds(first, span)
            seen = pl.ds(0, first + span)
            query_rows = jnp.where(mask, q_b[near, tile], jnp.zeros((), BF16))
            value = scores(query_rows, k_b[seen, tile], first)
            log_total = norm_log[head, near, :][:, :1]
            chances = jnp.exp(value - log_total)
            part_v = dot(gat[mine, near], chances.astype(BF16))
            grad_rows = jnp.where(mask, g_att[near, tile], jnp.zeros((), BF16))
            grad_chances = dot(grad_rows, v_b[seen, tile], NT)
            inner_sum = jnp.sum(chances * grad_chances, axis=-1, keepdims=True)
            grad_scores = (chances * (grad_chances - inner_sum)).astype(BF16)
            part_q = dot(grad_scores, k_b[seen, tile]) * scale
            part_q = part_q.astype(BF16).astype(F32)
            old = gpr[near, tile].astype(F32)
            gpr[near, tile] = jnp.where(mask, part_q, old).astype(BF16)
            part_k = dot(qt[mine, near], grad_scores) * scale
            if first == 0:
                gkt[mine, pl.ds(0, span)] = part_k
                gvt[mine, pl.ds(0, span)] = part_v
            else:
                gkt[mine, pl.ds(0, span)] += part_k[:, :span]
                gvt[mine, pl.ds(0, span)] += part_v[:, :span]
                gkt[mine, pl.ds(span, span)] = part_k[:, span:]
                gvt[mine, pl.ds(span, span)] = part_v[:, span:]

    gpr[:, pl.ds(0, inner)] = jnp.zeros((tokens, inner), BF16)
    per_half = HEADS // SEQ_PARTS // 2
    loop(per_half, backward_head)
    gu_grad.relay_end(1)
    loop(per_half, lambda head: backward_head(head + per_half))

    def settle(index):
        tile = block(index, 128)
        for kind, source in ((1, gkt), (2, gvt)):
            value = source[tile, :].astype(BF16).T
            gpr[:, pl.ds(pl.multiple_of(kind * inner + index * 128, 128), 128)] = value

    loop(inner // 128, settle)

    def unturn(index):
        tile = block(index, 128)
        value = gpr[:, tile].astype(F32)
        gpr[:, tile] = (
            value * cos_ref[...] + turned_back(value * sin_ref[...])
        ).astype(BF16)

    loop(2 * inner // 128, unturn)
    qkv_grad = ColumnReduce(qkv_o, qkv_k, qkv_x, qkv_h, qkv_z, send, recv, take(12))
    qkv_grad.start(n1t, gpr)
    gu_grad.relay_mid(0)
    gu_grad.relay_end(2)
    mid_move.drain()
    gn1_move = seq_reduce(0, take(2))
    gn1_move.start(gpr, wqkv, NT)
    down_chain.total()
    gn1_move.relay()
    wout_grad.hand_on(1)
    gu_grad.relay_mid(1)
    gu_grad.relay_mid(2)
    down_move.finish()
    out_move.arrive()

    def emit(rows_now):
        out_stage[rows_now, :] = (mid[rows_now, :] + out_move.total(rows_now)).astype(BF16)

    over_rows(rows, 16, emit)
    finals = [pltpu.make_async_copy(out_stage, out, local.at[18])]
    finals[0].start()
    qkv_grad.relay_end(0)
    gn1_move.arrive()

    def first_back(rows_now):
        here = pl.ds(pl.multiple_of(part * rows + rows_now.start, 16), 16)
        pulled, summand = rms_back(
            x_all[here, :].astype(F32), gn1_move.total(rows_now), gain_one
        )
        in_stage[rows_now, :] = gmid[rows_now, :] + pulled
        gain_sum[pl.ds(0, 8), :] += jnp.sum(summand.reshape(2, 8, width), axis=0)

    over_rows(rows, 16, first_back)

    finals.append(pltpu.make_async_copy(in_stage, grad_in, local.at[28]))
    finals[-1].start()

    vector[...] = jnp.zeros_like(vector)
    first_gain = jnp.sum(gain_sum[pl.ds(0, 8), :], axis=0, keepdims=True)
    second_gain = jnp.sum(gain_sum[pl.ds(8, 8), :], axis=0, keepdims=True)
    for shard in range(Z_LEN * X_LEN):
        vector[pl.ds(shard * 8, 1), :] = first_gain[:, shard * 128 : shard * 128 + 128]
        vector[pl.ds(shard * 8 + 1, 1), :] = second_gain[:, shard * 128 : shard * 128 + 128]
    for kind in range(3):
        for piece in range(inner // 128):
            column = kind * inner + piece * 128
            row = kind * (width // 128) + quarter * (inner // 128) + piece
            vector[pl.ds(lax.div(row, 3) * 8 + 2 + lax.rem(row, 3), 1), :] = jnp.sum(
                gpr[:, column : column + 128].astype(F32), axis=0, keepdims=True
            )
    vector_move = VectorReduce(vector, seq_box, dp_box, vec_out, send, recv, take(12))
    vector_move.start()
    wout_grad.hand_on(2)
    gu_grad.arrive()

    def gu_sum(rows_now):
        value = gu_grad.total(rows_now)
        gu_stage[rows_now, :] = value[:, : 2 * whole]
        tail_box[pl.ds(pl.multiple_of(part * rows + rows_now.start, 16), 16), :] = value[:, 2 * whole :]

    over_rows(gu_grad.rows, 16, gu_sum)
    shares = [
        Share(
            gu_stage.at[:, pl.ds(kind * whole, whole)],
            lambda p, target=target: target.at[:, pl.ds(gate_start(quarter_of(p)), whole)],
            send, recv, local.at[19 + kind], take(3),
        )
        for kind, target in enumerate((o_gate, o_up))
    ]
    tail_move = SeqGather(tail_box, send, recv, take(3))
    tail_move.start()
    for share in shares:
        share.start()
    wout_grad.total(True)
    qkv_grad.relay_end(1)
    down_move.pass_on()
    qkv_grad.relay_mid(0)
    qkv_grad.relay_end(2)
    down_chain.finish(True)
    qkv_grad.relay_mid(1)
    qkv_grad.relay_mid(2)
    down_chain.finish(False)
    wout_grad.finish(True)
    wout_grad.total(False)
    vector_move.relay()
    tail_move.relay()
    for share in shares:
        share.relay()
    wout_grad.finish(False)
    qkv_grad.arrive()

    def qkv_sum(rows_now):
        qkv_stage[rows_now, :] = qkv_grad.total(rows_now)

    over_rows(qkv_grad.rows, 16, qkv_sum)
    for kind in range(3):
        share = Share(
            qkv_stage.at[:, pl.ds(kind * inner, inner)],
            lambda p, kind=kind: o_qkv.at[
                :, pl.ds(pl.multiple_of(kind * width + quarter_of(p) * inner, 128), inner)
            ],
            send, recv, local.at[21 + kind], take(3),
        )
        share.start()
        shares.append(share)
    tail_move.arrive()
    low = lanes(rows) < half
    order = [0, 2, 3, 1]
    for pair in range(2):
        even = tail_box[pl.ds(order[2 * pair] * rows, rows), :].astype(F32)
        uneven = tail_box[pl.ds(order[2 * pair + 1] * rows, rows), :].astype(F32)
        spot = pl.ds(pair * 2 * ff_part + whole, 128)
        edges[2 * pair] = jnp.where(low, even, pltpu.roll(uneven, half, axis=1)).astype(BF16)
        edges[2 * pair + 1] = jnp.where(low, pltpu.roll(even, half, axis=1), uneven).astype(BF16)
        for kind, target in enumerate((o_gate, o_up)):
            index = 2 * pair + kind
            final = pltpu.make_async_copy(edges.at[index], target.at[:, spot], local.at[24 + index])
            final.start()
            finals.append(final)
    down_chain.pass_on()
    wout_grad.pass_on()
    for share in shares[2:]:
        share.relay()
    vector_move.finish()
    for share in shares:
        share.finish()
    for final in finals:
        final.wait()
    assert used[0] == SEMAPHORES, used[0]
    for move in (
        x_move, cot_move, small_move, qkv_move, wout_move, gu_move, wdown_move,
        n2_move, gn2_move, out_move, gb_move, gn1_move,
        down_move, down_chain, gu_grad, wout_grad, qkv_grad, vector_move, tail_move,
    ):
        move.drain()


def rope_constants(tokens):
    steps = np.arange(0, HEAD_DIM, 2).astype(np.float32) / np.float32(HEAD_DIM)
    inverse_freq = (1.0 / np.float32(ROPE_BASE) ** steps).astype(np.float32)
    angles = np.arange(tokens).astype(np.float32)[:, None] * inverse_freq[None, :]
    return [np.tile(table(angles).astype(np.float32), (1, 4)) for table in (np.cos, np.sin)]


WIDEN_STEPS = 2


def widen_kernel(*refs):
    sums, sources, refs = refs[0], refs[1:8], refs[8:]
    (gain_one, bias, gain_two), targets, refs = refs[:3], refs[3:10], refs[10:]
    wide, narrow, (sem_in, sem_out) = refs[:7], refs[7:12], refs[12:]
    gain_one[...] = sums[pl.ds(0, 1), :]
    gain_two[...] = sums[pl.ds(1, 1), :]
    for row in range(3):
        bias[pl.ds(row * 128, 128)] = sums[2 + row]

    def pieces(index):
        rows = sources[index].shape[0] // WIDEN_STEPS
        for step in range(WIDEN_STEPS):
            yield step, pl.ds(step * rows, rows)

    def fetch(index, step, rows):
        target = wide[index] if index < 2 else narrow[index - 2]
        return pltpu.make_async_copy(
            sources[index].at[rows], target.at[rows], sem_in.at[index, step]
        )

    def store(index, step, rows):
        return pltpu.make_async_copy(
            wide[index].at[rows], targets[index].at[rows], sem_out.at[index, step]
        )

    order = (2, 3, 4, 5, 6, 0, 1)
    for index in order:
        for step, rows in pieces(index):
            fetch(index, step, rows).start()
    for index in order:
        for step, rows in pieces(index):
            fetch(index, step, rows).wait()
            if index > 1:
                wide[index][rows, :] = narrow[index - 2][rows, :].astype(F32)
            store(index, step, rows).start()
    for index in order:
        for step, rows in pieces(index):
            store(index, step, rows).wait()


def widen(out, grad_in, sums, *bulk):
    def like(array, dtype=F32):
        return jax.ShapeDtypeStruct(array.shape, dtype)

    one, bias = jax.ShapeDtypeStruct((1, 128), F32), jax.ShapeDtypeStruct((384,), F32)
    results = pl.pallas_call(
        widen_kernel,
        out_shape=(one, bias, one, like(out, BF16), like(grad_in)) + tuple(map(like, bulk)),
        in_specs=[VMEM] + [HBM] * 7,
        out_specs=[VMEM] * 3 + [HBM] * 7,
        scratch_shapes=[pltpu.VMEM(out.shape, BF16), pltpu.VMEM(grad_in.shape, F32)]
        + [pltpu.VMEM(each.shape, F32) for each in bulk]
        + [pltpu.VMEM(each.shape, BF16) for each in bulk]
        + [pltpu.SemaphoreType.DMA((7, WIDEN_STEPS))] * 2,
    )(sums, out, grad_in, *bulk)
    gain_one, bias, gain_two, out, grad_in, g_qkv, g_out, g_gate, g_up, g_down = results
    return (
        out, grad_in, gain_one.reshape(-1), g_qkv, bias, g_out, gain_two.reshape(-1),
        g_gate, g_up, g_down,
    )


def ring_body(inputs, gain_attn, w_qkv, b_qkv, w_out, gain_mlp, w_gate, w_up, w_down, cotangent):
    rows, width = inputs.shape
    count = Z_LEN * X_LEN
    inner = HEADS // SEQ_PARTS * HEAD_DIM
    ff_part = w_gate.shape[1] // SEQ_PARTS
    padded = (ff_part + 127) // 128 * 128
    tokens = rows * SEQ_PARTS
    cos_two, sin_two = [jnp.asarray(table) for table in rope_constants(tokens)]

    def vm(*shape, dtype=BF16):
        return pltpu.VMEM(shape, dtype)

    gu_wide, qkv_wide = 2 * ff_part, 3 * inner
    down_rows, out_rows, shard = w_down.shape[0], w_out.shape[0], w_qkv.shape[0]
    scratch = [
        vm(tokens, width), vm(tokens, width), vm(count * 8, 128, dtype=F32),
        vm(8, width, dtype=F32), vm(24, 128, dtype=F32), vm(2, shard, 128),
        vm(width, qkv_wide), vm(inner, width), vm(width, gu_wide), vm(padded + 64, width),
        vm(tokens, width), vm(width, tokens), vm(tokens, width), vm(width, tokens),
        vm(tokens, width), vm(tokens, inner), vm(tokens, inner), vm(tokens, inner),
        vm(inner, tokens), vm(tokens, inner), vm(inner, tokens),
        vm(HEADS // SEQ_PARTS, tokens, 128, dtype=F32), vm(rows, width, dtype=F32),
        vm(tokens, gu_wide, dtype=F32), vm(tokens, padded), vm(padded, tokens),
        vm(tokens, gu_wide), vm(ff_part, width, dtype=F32), vm(inner, width, dtype=F32),
        vm(tokens, inner), vm(inner, tokens), vm(tokens, qkv_wide),
        vm(inner, tokens, dtype=F32), vm(inner, tokens, dtype=F32), vm(rows, width, dtype=F32),
    ]
    scratch += [vm(tokens, 128, dtype=F32)] * 2
    scratch += [vm(3, rows, width, dtype=F32)] * 2
    scratch += [vm(3, 2, rows, width, dtype=F32)] * 2
    scratch += [vm(3, rows, width)] * 2
    part_rows = down_rows // 2
    scratch += [vm(down_rows, width), vm(2, down_rows, width)] + [vm(part_rows, width)] * 2
    scratch += [vm(part_rows, width)] * 3 + [vm(Z_LEN - 1, part_rows, width)]
    scratch += [
        vm(Z_LEN, shard, gu_wide), vm(Z_LEN, shard, gu_wide, dtype=F32), vm(Z_LEN, shard, gu_wide),
        vm(Z_LEN - 1, shard, gu_wide), vm(Z_LEN + 1, shard, gu_wide),
    ]
    scratch += [vm(inner, width), vm(out_rows, width), vm(out_rows, width)]
    scratch += [vm(2, inner, width)]
    scratch += [
        vm(Z_LEN, shard, qkv_wide), vm(Z_LEN, shard, qkv_wide, dtype=F32), vm(Z_LEN, shard, qkv_wide),
        vm(Z_LEN - 1, shard, qkv_wide), vm(Z_LEN + 1, shard, qkv_wide),
    ]
    scratch += [
        vm(SEQ_PARTS * shard, 128), vm(shard, gu_wide - 128), vm(shard, qkv_wide), vm(rows, width),
        vm(rows, width, dtype=F32), vm(4, shard, 128), vm(16, width, dtype=F32), vm(count * 8, 128, dtype=F32),
        vm(SEQ_PARTS, count * 8, 128, dtype=F32), vm(count, 8, 128, dtype=F32),
        pltpu.SemaphoreType.DMA((SEMAPHORES,)), pltpu.SemaphoreType.DMA((SEMAPHORES,)),
        pltpu.SemaphoreType.DMA((30,)),
    ]
    output, grad_inputs, sums, g_qkv, g_out, g_gate, g_up, g_down = pl.pallas_call(
        layer_kernel,
        out_shape=(
            jax.ShapeDtypeStruct((rows, width), BF16),
            jax.ShapeDtypeStruct((rows, width), F32),
            jax.ShapeDtypeStruct((8, 128), F32),
            jax.ShapeDtypeStruct(w_qkv.shape, BF16),
            jax.ShapeDtypeStruct(w_out.shape, BF16),
            jax.ShapeDtypeStruct(w_gate.shape, BF16),
            jax.ShapeDtypeStruct(w_up.shape, BF16),
            jax.ShapeDtypeStruct(w_down.shape, BF16),
        ),
        in_specs=[HBM] * 9 + [VMEM] * 3,
        out_specs=[HBM] * 2 + [VMEM] + [HBM] * 5,
        scratch_shapes=scratch,
        compiler_params=pltpu.CompilerParams(
            collective_id=0, has_side_effects=True, vmem_limit_bytes=67043328
        ),
    )(
        inputs, cotangent, w_qkv, w_out, w_gate, w_up, w_down, cos_two, sin_two,
        gain_attn.reshape(1, 128), gain_mlp.reshape(1, 128), b_qkv.reshape(3, 128),
    )
    return widen(output, grad_inputs, sums, g_qkv, g_out, g_gate, g_up, g_down)


def solution(mesh):
    tuned = mesh.shape["dp"] == Z_LEN * X_LEN and mesh.shape["seq"] == SEQ_PARTS
    return jax.shard_map(
        ring_body if tuned else generic_body,
        mesh=mesh,
        in_specs=(
            P(("dp", "seq"), None),
            P("dp"),
            P("dp", None),
            P("dp"),
            P("dp", None),
            P("dp"),
            P("dp", None),
            P("dp", None),
            P("dp", None),
            P(("dp", "seq"), None),
        ),
        out_specs=(
            P(("dp", "seq"), None),
            P(("dp", "seq"), None),
            P("dp"),
            P("dp", None),
            P("dp"),
            P("dp", None),
            P("dp"),
            P("dp", None),
            P("dp", None),
            P("dp", None),
        ),
        check_vma=False,
    )
```
